512 devices in a mesh: parts: 2 (over y), space: 32 (over z), tm: 4 (over x), spin: 2 (over core).
Axes of the slice: x: 4, y: 2, z: 32, core: 2. Of those that a mesh axis runs over, the one named last changes fastest.
The devices are a block of a 4x8x32 slice.
Arguments:
- backward: bfloat16 [4, 4, 4, 64, 3, 32, 128], P('parts', 'tm', None, 'spin', None, 'space'), parts along dimension 0, may hold values from -6 to 6
- forward: bfloat16 [4, 4, 4, 64, 3, 32, 128], P('parts', 'tm', None, 'spin', None, 'space'), parts along dimension 0, may hold values from -6 to 6
- gauge_links: bfloat16 [4, 3, 3, 3, 4, 32, 128], P('parts', None, None, None, 'tm', 'space'), parts along dimension 0, may hold values from -2.5 to 2.5
- momenta: int32 [3, 3], replicated, may hold values from -2 to 2
- gamma_list: int32 [16], replicated, may hold values from 0 to 15
Outputs:
- insertion: float32 [4, 3, 16, 4, 64, 64], P('parts', None, None, 'tm', 'space', 'spin'), parts along dimension 0
The draws below stay inside these ranges and needn't reach their ends.
There are 2 independent parts, one for each index of `parts`. The reference program is written for one: setup_inputs(seed, part) draws one part's arguments, and reference() takes and returns one part's arrays. A program takes and returns all parts, laid end to end along the dimension named above; an argument that names none is the same for every part. Nothing has to cross between parts.
All inputs are finite; a program needn't handle non-finite values.
Results may differ from the reference program's by a relative error of at most 0.0056.
Values may be sent and summed in bfloat16 or wider, within the bound.
A program may use at most 64 MiB of HBM per device.

```python
import math
import jax
import jax.numpy as jnp
import numpy as np
from jax import lax

LX = 32
LY = 4
NCOL = 64
NGAM = 16
NMOM = 3
LZ = 32
SLAB = 4


def with_ends(values, rng, low, top_value):
    index_at = [jax.random.randint(jax.random.fold_in(rng, axis), (), 0, length) for axis, length in enumerate(values.shape)]
    widest = values.shape.index(max(values.shape))
    neighbour = index_at[:widest] + [(index_at[widest] + 1) % values.shape[widest]] + index_at[widest + 1:]
    return values.at[tuple(index_at)].set(low).at[tuple(neighbour)].set(top_value)


def block_scale(stream_key, extent, cuts, low, high):
    factor_of = 1.0
    for axis_at, parts in cuts:
        draws = jax.random.uniform(jax.random.fold_in(jax.random.fold_in(stream_key, 6), axis_at), (parts,), jnp.float32, low / len(cuts), high / len(cuts))
        factor_of = factor_of * jnp.repeat(jnp.exp(draws), extent[axis_at] // parts).reshape((-1,) + (1,) * (len(extent) - 1 - axis_at))
    return factor_of


def bell_draw(rng, extent, width, reach, split=(), kind=jnp.bfloat16):
    entries = width * jax.random.normal(rng, extent, jnp.float32)
    if split:
        entries = entries * block_scale(rng, extent, split, -0.22, 0.18)
    return jnp.clip(entries, -reach, reach).astype(kind)


def setup_inputs(seed: int = 0, part: int = 0) -> dict:
    splits = jax.random.split(jax.random.key(seed), 6)
    own_keys = jax.random.split(jax.random.fold_in(splits[5], part), 6)
    return {
        "backward": bell_draw(own_keys[0], (2, SLAB, 4, NCOL, 3, LZ, LX * LY), 1.0, 6.0, ((1, 4), (3, 2), (5, 32))),
        "forward": bell_draw(own_keys[1], (2, SLAB, 4, NCOL, 3, LZ, LX * LY), 1.0, 6.0, ((1, 4), (3, 2), (5, 32))),
        "gauge_links": bell_draw(own_keys[2], (2, 3, 3, 3, SLAB, LZ, LX * LY), 0.41, 2.5, ((4, 4), (5, 32))),
        "momenta": with_ends(jax.random.randint(splits[3], (NMOM, 3), -2, 3), jax.random.fold_in(splits[3], 1), -2, 2).astype(jnp.int32),
        "gamma_list": with_ends(jax.random.randint(splits[4], (NGAM,), 0, 16), jax.random.fold_in(splits[4], 1), 0, 15).astype(jnp.int32),
    }


def gamma_tables():
    zeros = np.zeros((4, 4))
    gx_imag = np.array([[0, 0, 0, 1], [0, 0, 1, 0], [0, -1, 0, 0], [-1, 0, 0, 0]]) * 1.0
    gy_real = np.array([[0, 0, 0, -1], [0, 0, 1, 0], [0, 1, 0, 0], [-1, 0, 0, 0]]) * 1.0
    gz_imag = np.array([[0, 0, 1, 0], [0, 0, 0, -1], [-1, 0, 0, 0], [0, 1, 0, 0]]) * 1.0
    gt_real = np.array([[0, 0, 1, 0], [0, 0, 0, 1], [1, 0, 0, 0], [0, 1, 0, 0]]) * 1.0
    singles = [(zeros, gx_imag), (gy_real, zeros), (zeros, gz_imag), (gt_real, zeros)]
    clif_real = []
    clif_imag = []
    for number in range(16):
        mat_real = np.eye(4)
        mat_imag = np.zeros((4, 4))
        for which in range(4):
            if number >> which & 1:
                other_real, other_imag = singles[which]
                new_real = mat_real @ other_real - mat_imag @ other_imag
                new_imag = mat_real @ other_imag + mat_imag @ other_real
                mat_real, mat_imag = (new_real, new_imag)
        clif_real.append(mat_real)
        clif_imag.append(mat_imag)
    return (singles, (np.stack(clif_real), np.stack(clif_imag)))

def chosen_gammas(gamma_list):
    singles, clifford = gamma_tables()
    table_real = jnp.asarray(clifford[0], dtype=jnp.float32)
    table_imag = jnp.asarray(clifford[1], dtype=jnp.float32)
    one_hot = (gamma_list[:, None] == jnp.arange(16, dtype=jnp.int32)[None, :]).astype(jnp.float32)
    gam_real = jnp.einsum('kg,gsv->ksv', one_hot, table_real, precision=lax.Precision.HIGHEST)
    gam_imag = jnp.einsum('kg,gsv->ksv', one_hot, table_imag, precision=lax.Precision.HIGHEST)
    return (gam_real, gam_imag)

def color_apply(link_real, link_imag, spin_real, spin_imag, dagger):
    outs_real = []
    outs_imag = []
    for c in range(3):
        summed_real = 0.0
        summed_imag = 0.0
        for d in range(3):
            if dagger:
                coef_real = link_real[d, c]
                coef_imag = -link_imag[d, c]
            else:
                coef_real = link_real[c, d]
                coef_imag = link_imag[c, d]
            coef_real = coef_real[..., None, None, :, :]
            coef_imag = coef_imag[..., None, None, :, :]
            part_real = spin_real[..., d, :, :]
            part_imag = spin_imag[..., d, :, :]
            summed_real = summed_real + coef_real * part_real - coef_imag * part_imag
            summed_imag = summed_imag + coef_real * part_imag + coef_imag * part_real
        outs_real.append(summed_real)
        outs_imag.append(summed_imag)
    return (jnp.stack(outs_real, axis=-3), jnp.stack(outs_imag, axis=-3))

def spin_apply(matrix, spin_real, spin_imag):
    outs_real = []
    outs_imag = []
    for t in range(4):
        summed_real = 0.0
        summed_imag = 0.0
        for s in range(4):
            coef_real = float(matrix[0][t, s])
            coef_imag = float(matrix[1][t, s])
            if coef_real == 0.0 and coef_imag == 0.0:
                continue
            part_real = spin_real[..., s, :, :, :, :]
            part_imag = spin_imag[..., s, :, :, :, :]
            summed_real = summed_real + coef_real * part_real - coef_imag * part_imag
            summed_imag = summed_imag + coef_real * part_imag + coef_imag * part_real
        outs_real.append(summed_real)
        outs_imag.append(summed_imag)
    return (jnp.stack(outs_real, axis=-5), jnp.stack(outs_imag, axis=-5))

def plane_roll(spinor, offset, along_y, width_x):
    initial = spinor.shape
    gridded = spinor.reshape(initial[:-1] + (initial[-1] // width_x, width_x))
    gridded = jnp.roll(gridded, offset, axis=-2 if along_y else -1)
    return gridded.reshape(initial)

def current(fwd_real, fwd_imag, link_real, link_imag, up_z, down_z, width_x):
    singles, clifford = gamma_tables()
    summed_real = 0.0
    summed_imag = 0.0
    for direction in range(3):
        single_real, single_imag = singles[direction]
        minus_proj = ((np.eye(4) - single_real) / 2.0, -single_imag / 2.0)
        plus_proj = ((np.eye(4) + single_real) / 2.0, single_imag / 2.0)
        if direction < 2:
            along_y = direction == 1
            up_real = plane_roll(fwd_real, -1, along_y, width_x)
            up_imag = plane_roll(fwd_imag, -1, along_y, width_x)
            back_real, back_imag = color_apply(link_real[direction], link_imag[direction], fwd_real, fwd_imag, True)
            down_real = plane_roll(back_real, 1, along_y, width_x)
            down_imag = plane_roll(back_imag, 1, along_y, width_x)
        else:
            up_real, up_imag = up_z
            down_real, down_imag = down_z
        hop_real, hop_imag = color_apply(link_real[direction], link_imag[direction], up_real, up_imag, False)
        ahead_real, ahead_imag = spin_apply(minus_proj, hop_real, hop_imag)
        behind_real, behind_imag = spin_apply(plus_proj, down_real, down_imag)
        summed_real = summed_real + ahead_real - behind_real
        summed_imag = summed_imag + ahead_imag - behind_imag
    return (summed_real, summed_imag)

def phase_list(momenta, z_start, layers, plane_size, width_x, width_y, full_z):
    sites = jnp.arange(plane_size, dtype=jnp.int32)
    coord_x = sites % width_x
    coord_y = sites // width_x
    coord_z = z_start + jnp.arange(layers, dtype=jnp.int32)
    result = []
    for number in range(momenta.shape[0]):
        frac_plane = jnp.mod(momenta[number, 0] * coord_x, width_x).astype(jnp.float32) / float(width_x)
        frac_plane = frac_plane + jnp.mod(momenta[number, 1] * coord_y, width_y).astype(jnp.float32) / float(width_y)
        frac_depth = jnp.mod(momenta[number, 2] * coord_z, full_z).astype(jnp.float32) / float(full_z)
        result.append(2.0 * math.pi * (frac_depth[:, None] + frac_plane[None, :]))
    return result

def contract(back_piece, weave_re, weave_im, thetas, gam_real, gam_imag, scaling):
    back_real = back_piece[0].astype(jnp.float32)
    back_imag = back_piece[1].astype(jnp.float32)
    slab_times, spins, columns = (back_real.shape[0], back_real.shape[1], back_real.shape[2])
    blocks = []
    for theta in thetas:
        cosine = jnp.cos(theta)
        sine_part = jnp.sin(theta)
        rot_real = lax.optimization_barrier((cosine * back_real - sine_part * back_imag).astype(jnp.bfloat16)).astype(jnp.float32)
        rot_imag = lax.optimization_barrier((sine_part * back_real + cosine * back_imag).astype(jnp.bfloat16)).astype(jnp.float32)
        stacked = jnp.concatenate([rot_real.reshape(slab_times, spins, columns, -1), rot_imag.reshape(slab_times, spins, columns, -1)], axis=-1)
        pair_real = jnp.einsum('usak,uvbk->usvab', stacked, weave_re)
        pair_imag = jnp.einsum('usak,uvbk->usvab', stacked, weave_im)
        out_real = jnp.einsum('ksv,usvab->kuab', gam_real, pair_real, precision=lax.Precision.HIGHEST) - jnp.einsum('ksv,usvab->kuab', gam_imag, pair_imag, precision=lax.Precision.HIGHEST)
        out_imag = jnp.einsum('ksv,usvab->kuab', gam_real, pair_imag, precision=lax.Precision.HIGHEST) + jnp.einsum('ksv,usvab->kuab', gam_imag, pair_real, precision=lax.Precision.HIGHEST)
        blocks.append(jnp.stack([out_real, out_imag]) * scaling)
    return jnp.stack(blocks, axis=1)

def reference(backward, forward, gauge_links, momenta, gamma_list):
    layers = forward.shape[5]
    plane_size = forward.shape[6]
    width_x = LX
    thetas = phase_list(momenta, jnp.int32(0), layers, plane_size, width_x, plane_size // width_x, layers)
    gam_real, gam_imag = chosen_gammas(gamma_list)
    scaling = 1.0 / math.sqrt(3.0 * plane_size * layers)

    def one_time(slices):
        back_slice, fwd_slice, link_slice = slices
        fwd_real = fwd_slice[0][None].astype(jnp.float32)
        fwd_imag = fwd_slice[1][None].astype(jnp.float32)
        link_real = link_slice[0][:, :, :, None].astype(jnp.float32)
        link_imag = link_slice[1][:, :, :, None].astype(jnp.float32)
        up_z = (jnp.roll(fwd_real, -1, axis=-2), jnp.roll(fwd_imag, -1, axis=-2))
        back_real, back_imag = color_apply(link_real[2], link_imag[2], fwd_real, fwd_imag, True)
        down_z = (jnp.roll(back_real, 1, axis=-2), jnp.roll(back_imag, 1, axis=-2))
        weave_real, weave_imag = current(fwd_real, fwd_imag, link_real, link_imag, up_z, down_z, width_x)
        woven_real = lax.optimization_barrier(weave_real.astype(jnp.bfloat16)).astype(jnp.float32)
        woven_imag = lax.optimization_barrier(weave_imag.astype(jnp.bfloat16)).astype(jnp.float32)
        flat_real = woven_real.reshape(woven_real.shape[0], 4, woven_real.shape[2], -1)
        flat_imag = woven_imag.reshape(woven_imag.shape[0], 4, woven_imag.shape[2], -1)
        weave_re = jnp.concatenate([flat_real, flat_imag], axis=-1)
        weave_im = jnp.concatenate([flat_imag, -flat_real], axis=-1)
        result = contract(back_slice[:, None], weave_re, weave_im, thetas, gam_real, gam_imag, scaling)
        return result[:, :, :, 0]
    stacked = lax.map(one_time, (jnp.moveaxis(backward, 1, 0), jnp.moveaxis(forward, 1, 0), jnp.moveaxis(gauge_links, 4, 0)))
    return jnp.moveaxis(stacked, 0, 3)
```

```python
import functools
import math

import jax
import jax.numpy as jnp
import numpy as np
from jax import lax
from jax.experimental import pallas as pl
from jax.experimental.pallas import tpu as pltpu
from jax.sharding import PartitionSpec as P

MESH = pl.DeviceIdType.MESH
LX = 32
F32 = jnp.float32
BF16 = jnp.bfloat16

CENTERS = {-8: (-7, -9), -11: (-10, -12), -14: (-13, -15), 4: (3, 5), 7: (6, 8), 10: (9, 11), 13: (12, 14), 16: (15,)}
DIRECT = (-1, -2, -3, -4, -5, -6, 1, 2)
CENTER_ORDER = (4, 7, 10, 13, 16, -8, -11, -14)
CHILD = tuple((child, q) for q in CENTER_ORDER for child in CENTERS[q])
OFFSETS = DIRECT + tuple(c for c, _ in CHILD) + CENTER_ORDER
SLOT = {o: i for i, o in enumerate(OFFSETS)}


def gamma_tables():
    zeros = np.zeros((4, 4))
    gx = np.array([[0, 0, 0, 1j], [0, 0, 1j, 0], [0, -1j, 0, 0], [-1j, 0, 0, 0]])
    gy = np.array([[0, 0, 0, -1], [0, 0, 1, 0], [0, 1, 0, 0], [-1, 0, 0, 0]]) + 0j
    gz = np.array([[0, 0, 1j, 0], [0, 0, 0, -1j], [-1j, 0, 0, 0], [0, 1j, 0, 0]])
    gt = np.array([[0, 0, 1, 0], [0, 0, 0, 1], [1, 0, 0, 0], [0, 1, 0, 0]]) + 0j
    singles = [gx, gy, gz, gt]
    basis = []
    for number in range(16):
        mat = np.eye(4) + 0j
        for which in range(4):
            if number >> which & 1:
                mat = mat @ singles[which]
        basis.append(mat)
    return singles, np.stack(basis)


def contraction_table(nmom):
    _, basis = gamma_tables()
    table = np.zeros((2, 128, 256), np.float32)
    for g in range(16):
        for p in range(nmom):
            for a in range(2):
                row = g * 2 * nmom + p * 2 + a
                for s in range(4):
                    for s2 in range(4):
                        value = basis[g][s, s2]
                        for ri_out, ri_in, coef in ((0, 0, value.real), (0, 1, -value.imag), (1, 0, value.imag), (1, 1, value.real)):
                            table[ri_out, row, ((s2 * 2 + ri_in) * nmom + p) * 8 + s * 2 + a] = coef
    return table


def times_unit(coef, value):
    re, im = value
    if coef == 1:
        return re, im
    if coef == -1:
        return -re, -im
    if coef == 1j:
        return -im, re
    assert coef == -1j
    return im, -re


def plus(x, y):
    return x[0] + y[0], x[1] + y[1]


def projector(mu, sign):
    singles, _ = gamma_tables()
    mat = np.eye(4) + sign * singles[mu]
    result = []
    for s in range(2):
        t = [t for t in (2, 3) if mat[s, t] != 0][0]
        result.append((s, t, complex(mat[s, t]), complex(mat[t, s])))
    return result


def kernel(n, nmom, ngam, scaling,
           mom_ref, gam_ref, b_hbm, f_hbm, u_hbm, t_hbm, o_ref,
           fv, uv, tv, bb, ff, uf, bf, wv, lh, rh, rp, ck, hup_s, hup_r, hdn_s, hdn_r, cbuf, rbuf, cs, lmat,
           lsem, bsem, hsem, csend, crecv, ready, readyp):
    z = lax.axis_index("space")
    spin = lax.axis_index("spin")
    rows = fv.shape[3]

    load_f = pltpu.make_async_copy(f_hbm, fv, lsem.at[0])
    load_u = pltpu.make_async_copy(u_hbm, uv, lsem.at[1])
    load_b = pltpu.make_async_copy(b_hbm, bb.at[spin], lsem.at[2])
    load_t = pltpu.make_async_copy(t_hbm, tv, lsem.at[3])
    for copy in (load_f, load_u, load_b, load_t):
        copy.start()

    links = {1, n - 1} | {(-o) % n for o in DIRECT + CENTER_ORDER} | {o % n for o in DIRECT + CENTER_ORDER}
    links |= {(q - c) % n for c, q in CHILD} | {(c - q) % n for c, q in CHILD}
    peers = sorted(links)
    at = {d: i for i, d in enumerate(peers)}

    def chip(d):
        return {"space": lax.rem(z + d, n)}

    barrier = pltpu.get_barrier_semaphore()
    count = jnp.where(spin == 0, 1, 0)
    for d in peers:
        count = count + jnp.where(z + d >= n, 1, 0)

        @pl.when(z + d < n)
        def _():
            pl.semaphore_signal(barrier, inc=1, device_id=chip(d), device_id_type=MESH)

    @pl.when(spin == 1)
    def _():
        pl.semaphore_signal(barrier, inc=1, device_id={"spin": 0}, device_id_type=MESH)

    @pl.when(count > 0)
    def _():
        pl.semaphore_wait(barrier, count)

    for d in peers:
        @pl.when(z + d >= n)
        def _():
            pl.semaphore_signal(ready.at[at[n - d]], inc=1, device_id=chip(d), device_id_type=MESH)

    @pl.when(spin == 0)
    def _():
        pl.semaphore_signal(readyp, inc=1, device_id={"spin": 1}, device_id_type=MESH)

    seen = set()

    def reach(d):
        if d not in seen:
            seen.add(d)

            @pl.when(z + d < n)
            def _():
                pl.semaphore_wait(ready.at[at[d]], 1)

    load_f.wait()
    load_u.wait()
    ff[...] = fv[...].astype(F32)
    for i in range(uv.shape[0]):
        uf[i] = uv[i].astype(F32)

    def link(mu, c, d, dagger):
        if dagger:
            return uf[mu * 9 + d * 3 + c, 0:1, :], -uf[mu * 9 + d * 3 + c, 1:2, :]
        return uf[mu * 9 + c * 3 + d, 0:1, :], uf[mu * 9 + c * 3 + d, 1:2, :]

    def colored(mu, dagger, h):
        out = []
        for c in range(3):
            re = im = None
            for d in range(3):
                cr, ci = link(mu, c, d, dagger)
                hr, hi = h[d]
                pr, pi = cr * hr - ci * hi, cr * hi + ci * hr
                re, im = (pr, pi) if re is None else (re + pr, im + pi)
            out.append((re, im))
        return out

    def half(mu, sign, which, sl):
        s, t, alpha, beta = projector(mu, sign)[which]
        h = []
        for c in range(3):
            x = (ff[0, s, c, sl, :], ff[1, s, c, sl, :])
            y = (ff[0, t, c, sl, :], ff[1, t, c, sl, :])
            h.append(plus(x, times_unit(alpha, y)))
        return s, t, beta, h

    blocks = [pl.ds(i, 16) for i in range(0, rows, 16)]
    for which in range(2):
        for sl in blocks:
            _, _, _, h = half(2, -1, which, sl)
            for c in range(3):
                hup_s[0, which, c, sl, :] = h[c][0].astype(BF16)
                hup_s[1, which, c, sl, :] = h[c][1].astype(BF16)
    send_up = pltpu.make_async_remote_copy(hup_s, hup_r, hsem.at[0], hsem.at[1], device_id=chip(n - 1), device_id_type=MESH)
    for which in range(2):
        for sl in blocks:
            _, _, _, h = half(2, 1, which, sl)
            h = colored(2, True, h)
            for c in range(3):
                hdn_s[0, which, c, sl, :] = h[c][0].astype(BF16)
                hdn_s[1, which, c, sl, :] = h[c][1].astype(BF16)
    send_dn = pltpu.make_async_remote_copy(hdn_s, hdn_r, hsem.at[2], hsem.at[3], device_id=chip(1), device_id_type=MESH)

    @pl.when(z > 0)
    def _():
        send_up.start()

    @pl.when(z == n - 1)
    def _():
        send_dn.start()

    load_b.wait()

    @pl.when(spin == 1)
    def _():
        pl.semaphore_wait(readyp, 1)

    swap_b = pltpu.make_async_remote_copy(bb.at[spin], bb.at[spin], bsem.at[0], bsem.at[1], device_id={"spin": 1 - spin}, device_id_type=MESH)
    swap_b.start()

    @pl.when(z < n - 1)
    def _():
        pl.semaphore_wait(ready.at[at[1]], 1)
        send_dn.start()
    seen.add(1)

    sub = lax.broadcasted_iota(jnp.int32, (8, 128), 0)
    lane = lax.broadcasted_iota(jnp.int32, (8, 128), 1)
    x1, x2 = lane & (LX - 1), lane // LX
    width_y = 128 // LX

    def momentum(axis):
        value = jnp.full((8, 128), mom_ref[0, axis], jnp.int32)
        for p in range(1, nmom):
            value = jnp.where(sub == p, mom_ref[p, axis], value)
        return value

    turn = (((momentum(0) * x1) & (LX - 1)).astype(F32) / float(LX)
            + ((momentum(1) * x2) & (width_y - 1)).astype(F32) / float(width_y))
    turn = ((momentum(2) * z) & (n - 1)).astype(F32) / float(n) + turn
    theta = 2.0 * math.pi * turn
    cs[0] = jnp.cos(theta)
    cs[1] = jnp.sin(theta)

    first = lane[0:1, :] & (LX - 1)
    for mu in range(2):
        for which in range(2):
            for sl in blocks:
                for sign in (-1, 1):
                    s, t, beta, h = half(mu, sign, which, sl)
                    if sign == 1:
                        h = colored(mu, True, h)
                    moved = []
                    for pair in h:
                        if mu == 1:
                            moved.append(tuple(pltpu.roll(v, 128 - LX if sign == -1 else LX, 1) for v in pair))
                        elif sign == -1:
                            moved.append(tuple(jnp.where(first == LX - 1, pltpu.roll(v, LX - 1, 1), pltpu.roll(v, 127, 1)) for v in pair))
                        else:
                            moved.append(tuple(jnp.where(first == 0, pltpu.roll(v, 128 - (LX - 1), 1), pltpu.roll(v, 1, 1)) for v in pair))
                    h = moved
                    if sign == -1:
                        h = colored(mu, False, h)
                    for c in range(3):
                        other = times_unit(beta, h[c])
                        for ri in range(2):
                            if mu == 0 and sign == -1:
                                wv[ri, s, c, sl, :] = h[c][ri]
                                wv[ri, t, c, sl, :] = other[ri]
                            elif sign == -1:
                                wv[ri, s, c, sl, :] += h[c][ri]
                                wv[ri, t, c, sl, :] += other[ri]
                            else:
                                wv[ri, s, c, sl, :] -= h[c][ri]
                                wv[ri, t, c, sl, :] -= other[ri]

    load_t.wait()
    half_rows = nmom * ngam * 2
    r = lax.broadcasted_iota(jnp.int32, (half_rows, 128), 0)
    l2 = lax.broadcasted_iota(jnp.int32, (half_rows, 128), 1)
    k_of = (r >> 1) & (ngam - 1)
    p_of = r // (2 * ngam)
    g_of = jnp.full((half_rows, 128), gam_ref[0], jnp.int32)
    for k in range(1, ngam):
        g_of = jnp.where(k_of == k, gam_ref[k], g_of)
    hot = jnp.where(l2 == g_of * (2 * nmom) + p_of * 2 + (r & 1), 1.0, 0.0).astype(BF16)
    for ri in range(2):
        lmat[pl.ds(ri * half_rows, half_rows), :] = jnp.dot(hot, tv[ri], preferred_element_type=F32).astype(BF16)

    swap_b.wait_recv()
    bf[...] = bb[...].astype(F32)
    for s in range(4):
        for which in range(2):
            for c in range(3):
                for a in range(2):
                    br = bf.at[which, 0, s, c][pl.ds(a, 16, stride=2), :]
                    bi = bf.at[which, 1, s, c][pl.ds(a, 16, stride=2), :]
                    for p in range(nmom):
                        co, si = cs[0, p:p + 1, :], cs[1, p:p + 1, :]
                        at_row = pl.ds((p * 4 + s) * 64 + a * 32 + which * 16, 16)
                        lh[at_row, pl.ds(c * 128, 128)] = (co * br - si * bi).astype(BF16)
                        lh[at_row, pl.ds((3 + c) * 128, 128)] = (si * br + co * bi).astype(BF16)

    @pl.when(z == 0)
    def _():
        pl.semaphore_wait(ready.at[at[n - 1]], 1)
        send_up.start()
    seen.add(n - 1)

    send_up.wait_recv()
    for which in range(2):
        s, t, alpha, beta = projector(2, -1)[which]
        for sl in blocks:
            h = [(hup_r[0, which, c, sl, :].astype(F32), hup_r[1, which, c, sl, :].astype(F32)) for c in range(3)]
            h = colored(2, False, h)
            for c in range(3):
                other = times_unit(beta, h[c])
                for ri in range(2):
                    wv[ri, s, c, sl, :] += h[c][ri]
                    wv[ri, t, c, sl, :] += other[ri]
    send_dn.wait_recv()
    for which in range(2):
        s, t, alpha, beta = projector(2, 1)[which]
        for sl in blocks:
            start = sl.start
            for c in range(3):
                h = (hdn_r[0, which, c, sl, :].astype(F32), hdn_r[1, which, c, sl, :].astype(F32))
                other = times_unit(beta, h)
                for comp, value in ((s, h), (t, other)):
                    re = ((wv[0, comp, c, sl, :] - value[0]) * 0.5).astype(BF16)
                    im = ((wv[1, comp, c, sl, :] - value[1]) * 0.5).astype(BF16)
                    top, low = pl.ds(comp * rows + start, 16), pl.ds(4 * rows + comp * rows + start, 16)
                    rh[top, pl.ds(c * 128, 128)] = re
                    rh[top, pl.ds((3 + c) * 128, 128)] = im
                    rh[low, pl.ds(c * 128, 128)] = im
                    rh[low, pl.ds((3 + c) * 128, 128)] = -re

    for p in range(nmom):
        prod = lax.dot_general(lh[pl.ds(p * 256, 256), :], rh[...], (((1,), (1,)), ((), ())), preferred_element_type=F32)
        for j in range(8):
            for ri in range(2):
                rp[ri, pl.ds((p * 8 + j) * 40, 32), :] = prod[j * 32:(j + 1) * 32, ri * 128:(ri + 1) * 128]

    def partial(c):
        return [rp.at[ri][pl.ds(c, nmom * 8, stride=40), :] for ri in range(2)]

    def owner(o):
        return lax.rem(z + (-o) % n, n)

    copies = []

    def send(o, source, target):
        d = (target - o) % n
        reach(d)
        copy = pltpu.make_async_remote_copy(source, rbuf.at[SLOT[o]], csend.at[SLOT[o]], crecv.at[SLOT[o]], device_id=chip(d), device_id_type=MESH)
        copy.start()
        copies.append(copy)

    def arrived(o):
        pltpu.make_async_remote_copy(ck.at[0], rbuf.at[SLOT[o]], csend.at[SLOT[o]], crecv.at[SLOT[o]], device_id=chip(0), device_id_type=MESH).wait_recv()

    plain = [o for o in OFFSETS if o not in CENTERS]
    for i, o in enumerate(plain):
        ck[i] = jnp.concatenate(partial(owner(o)), axis=0).astype(BF16)
    for i, o in enumerate(plain):
        send(o, ck.at[i], dict(CHILD).get(o, 0))
    for i, q in enumerate(CENTER_ORDER):
        total = jnp.concatenate(partial(owner(q)), axis=0)
        for child in CENTERS[q]:
            arrived(child)
            total = total + rbuf[SLOT[child]].astype(F32)
        cbuf[i] = total.astype(BF16)
        send(q, cbuf.at[i], 0)

    total = jnp.concatenate(partial(z), axis=0)
    for o in DIRECT[6:] + CENTER_ORDER[:5] + CENTER_ORDER[:4:-1] + DIRECT[5::-1]:
        arrived(o)
        total = total + rbuf[SLOT[o]].astype(F32)
    stack = jnp.concatenate([total if s2 == 0 else pltpu.roll(total, 128 - s2 * rows, 1) for s2 in range(4)], axis=0)
    high = stack.astype(BF16)
    low = (stack - high.astype(F32)).astype(BF16)
    mat = lmat[:, 0:stack.shape[0]]
    out = jnp.dot(mat, high, preferred_element_type=F32) + jnp.dot(mat, low, preferred_element_type=F32)
    o_ref[...] = out[:, 0:rows] * scaling
    for d in peers:
        reach(d)
    for copy in copies:
        copy.wait_send()
    send_up.wait_send()
    send_dn.wait_send()
    swap_b.wait_send()


def solution(mesh):
    n = mesh.shape["space"]

    def body(backward, forward, gauge_links, momenta, gamma_list):
        cols, plane = forward.shape[3], forward.shape[6]
        nmom, ngam = momenta.shape[0], gamma_list.shape[0]
        scaling = 1.0 / math.sqrt(3.0 * plane * n)
        b = backward.transpose(0, 1, 2, 4, 5, 3, 6).reshape(2, 4, 3, cols, plane)
        f = forward.transpose(0, 1, 2, 4, 5, 3, 6).reshape(2, 4, 3, cols, plane)
        u = gauge_links.transpose(1, 2, 3, 4, 5, 0, 6).reshape(27, 2, plane)
        table = jnp.asarray(contraction_table(nmom), BF16)
        half_shape = (2, 2, 3, cols, plane)
        chunk = (nmom * 16, plane)
        n_rows = nmom * 4 * 2 * cols
        any_spec = pl.BlockSpec(memory_space=pl.ANY)
        smem = pl.BlockSpec(memory_space=pltpu.SMEM)
        n_links = len({1, n - 1} | {o % n for o in DIRECT + CENTER_ORDER} | {(-o) % n for o in DIRECT + CENTER_ORDER})
        out = pl.pallas_call(
            functools.partial(kernel, n, nmom, ngam, scaling),
            out_shape=jax.ShapeDtypeStruct((2 * nmom * ngam * 2, cols), F32),
            in_specs=[smem, smem, any_spec, any_spec, any_spec, any_spec],
            out_specs=pl.BlockSpec(memory_space=pltpu.VMEM),
            name="insertion",
            scratch_shapes=[
                pltpu.VMEM(f.shape, BF16),
                pltpu.VMEM(u.shape, BF16),
                pltpu.VMEM(table.shape, BF16),
                pltpu.VMEM((2, *b.shape), BF16),
                pltpu.VMEM(f.shape, F32),
                pltpu.VMEM(u.shape, F32),
                pltpu.VMEM((2, *b.shape), F32),
                pltpu.VMEM(f.shape, F32),
                pltpu.VMEM((n_rows, 6 * plane), BF16),
                pltpu.VMEM((8 * cols, 6 * plane), BF16),
                pltpu.VMEM((2, nmom * 8 * 40, plane), F32),
                pltpu.VMEM((len(OFFSETS) - len(CENTERS), *chunk), BF16),
                pltpu.VMEM(half_shape, BF16),
                pltpu.VMEM(half_shape, BF16),
                pltpu.VMEM(half_shape, BF16),
                pltpu.VMEM(half_shape, BF16),
                pltpu.VMEM((len(CENTERS), *chunk), BF16),
                pltpu.VMEM((len(OFFSETS), *chunk), BF16),
                pltpu.VMEM((2, 8, plane), F32),
                pltpu.VMEM((2 * nmom * ngam * 2, 256), BF16),
                pltpu.SemaphoreType.DMA((4,)),
                pltpu.SemaphoreType.DMA((2,)),
                pltpu.SemaphoreType.DMA((4,)),
                pltpu.SemaphoreType.DMA((len(OFFSETS),)),
                pltpu.SemaphoreType.DMA((len(OFFSETS),)),
                pltpu.SemaphoreType.REGULAR((n_links,)),
                pltpu.SemaphoreType.REGULAR,
            ],
            compiler_params=pltpu.CompilerParams(collective_id=0, has_side_effects=True, vmem_limit_bytes=67043328),
        )(momenta, gamma_list, b, f, u, table)
        return out.reshape(2, nmom, ngam, 1, 2, cols)

    in_specs = (
        P("parts", "tm", None, "spin", None, "space", None),
        P("parts", "tm", None, "spin", None, "space", None),
        P("parts", None, None, None, "tm", "space", None),
        P(),
        P(),
    )
    out_specs = P("parts", None, None, "tm", "space", "spin")
    return jax.shard_map(body, mesh=mesh, in_specs=in_specs, out_specs=out_specs, check_vma=False)
```

```python
import functools
import math

import jax
import jax.numpy as jnp
import numpy as np
from jax import lax
from jax.experimental import pallas as pl
from jax.experimental.pallas import tpu as pltpu
from jax.sharding import PartitionSpec as P

MESH = pl.DeviceIdType.MESH
LX = 32
F32 = jnp.float32
BF16 = jnp.bfloat16

STEP = 3


def gamma_tables():
    zeros = np.zeros((4, 4))
    gx = np.array([[0, 0, 0, 1j], [0, 0, 1j, 0], [0, -1j, 0, 0], [-1j, 0, 0, 0]])
    gy = np.array([[0, 0, 0, -1], [0, 0, 1, 0], [0, 1, 0, 0], [-1, 0, 0, 0]]) + 0j
    gz = np.array([[0, 0, 1j, 0], [0, 0, 0, -1j], [-1j, 0, 0, 0], [0, 1j, 0, 0]])
    gt = np.array([[0, 0, 1, 0], [0, 0, 0, 1], [1, 0, 0, 0], [0, 1, 0, 0]]) + 0j
    singles = [gx, gy, gz, gt]
    basis = []
    for number in range(16):
        mat = np.eye(4) + 0j
        for which in range(4):
            if number >> which & 1:
                mat = mat @ singles[which]
        basis.append(mat)
    return singles, np.stack(basis)


def contraction_table(nmom):
    _, basis = gamma_tables()
    table = np.zeros((2, 128, 256), np.float32)
    for g in range(16):
        for p in range(nmom):
            for a in range(2):
                row = g * 2 * nmom + p * 2 + a
                for s in range(4):
                    for s2 in range(4):
                        value = basis[g][s, s2]
                        for ri_out, ri_in, coef in ((0, 0, value.real), (0, 1, -value.imag), (1, 0, value.imag), (1, 1, value.real)):
                            table[ri_out, row, ((s2 * 2 + ri_in) * nmom + p) * 8 + s * 2 + a] = coef
    return table


def times_unit(coef, value):
    re, im = value
    if coef == 1:
        return re, im
    if coef == -1:
        return -re, -im
    if coef == 1j:
        return -im, re
    assert coef == -1j
    return im, -re


def plus(x, y):
    return x[0] + y[0], x[1] + y[1]


def projector(mu, sign):
    singles, _ = gamma_tables()
    mat = np.eye(4) + sign * singles[mu]
    result = []
    for s in range(2):
        t = [t for t in (2, 3) if mat[s, t] != 0][0]
        result.append((s, t, complex(mat[s, t]), complex(mat[t, s])))
    return result


def kernel(n, nmom, ngam, scaling,
           mom_hbm, gam_hbm, b_hbm, f_hbm, u_hbm, t_hbm, o_ref,
           fv, uv, tv, bb, ff, uf, bf, wv, lh, rh, rp, hup_s, hup_r, hdn_s, hdn_r, c1, c2, crole, r1, r2, r3, cs, lmat, mom_ref, gam_ref,
           lsem, bsem, hsem, csend, crecv, inside_sem, readyp):
    z = lax.axis_index("space")
    spin = lax.axis_index("spin")
    rows = fv.shape[3]

    load_f = pltpu.make_async_copy(f_hbm, fv, lsem.at[0])
    load_u = pltpu.make_async_copy(u_hbm, uv, lsem.at[1])
    load_b = pltpu.make_async_copy(b_hbm, bb.at[spin], lsem.at[2])
    load_t = pltpu.make_async_copy(t_hbm, tv, lsem.at[3])
    load_m = pltpu.make_async_copy(mom_hbm, mom_ref, lsem.at[4])
    load_g = pltpu.make_async_copy(gam_hbm, gam_ref, lsem.at[5])
    for copy in (load_f, load_u, load_b, load_t, load_m, load_g):
        copy.start()

    def chip(d):
        return {"space": lax.rem(z + d, n)}

    def tell(sem, d):
        pl.semaphore_signal(sem, inc=1, device_id=chip(d), device_id_type=MESH)

    up, down = 0, 1
    last = z == n - 1
    near_in, two_in, three_in = inside_sem.at[0], inside_sem.at[1], inside_sem.at[2]
    barrier = pltpu.get_barrier_semaphore()
    up_later = jnp.logical_and(z > 0, jnp.logical_not(last))
    down_later = z < 2

    @pl.when(up_later)
    def _():
        tell(barrier, 1)

    @pl.when(down_later)
    def _():
        tell(barrier, n - 1)

    @pl.when(spin == 1)
    def _():
        pl.semaphore_signal(barrier, inc=1, device_id={"spin": 0}, device_id_type=MESH)

    count = jnp.where(up_later, 0, 1) + jnp.where(down_later, 0, 1) + jnp.where(spin == 0, 1, 0)

    @pl.when(count > 0)
    def _():
        pl.semaphore_wait(barrier, count)

    @pl.when(jnp.logical_not(down_later))
    def _():
        tell(near_in.at[up], n - 1)

    @pl.when(jnp.logical_not(up_later))
    def _():
        tell(near_in.at[down], 1)

    @pl.when(spin == 0)
    def _():
        pl.semaphore_signal(readyp, inc=1, device_id={"spin": 1}, device_id_type=MESH)

    load_f.wait()
    load_u.wait()
    ff[...] = fv[...].astype(F32)
    for i in range(uv.shape[0]):
        uf[i] = uv[i].astype(F32)

    def link(mu, c, d, dagger):
        if dagger:
            return uf[mu * 9 + d * 3 + c, 0:1, :], -uf[mu * 9 + d * 3 + c, 1:2, :]
        return uf[mu * 9 + c * 3 + d, 0:1, :], uf[mu * 9 + c * 3 + d, 1:2, :]

    def colored(mu, dagger, h):
        out = []
        for c in range(3):
            re = im = None
            for d in range(3):
                cr, ci = link(mu, c, d, dagger)
                hr, hi = h[d]
                pr, pi = cr * hr - ci * hi, cr * hi + ci * hr
                re, im = (pr, pi) if re is None else (re + pr, im + pi)
            out.append((re, im))
        return out

    def half(mu, sign, which, sl):
        s, t, alpha, beta = projector(mu, sign)[which]
        h = []
        for c in range(3):
            x = (ff[0, s, c, sl, :], ff[1, s, c, sl, :])
            y = (ff[0, t, c, sl, :], ff[1, t, c, sl, :])
            h.append(plus(x, times_unit(alpha, y)))
        return s, t, beta, h

    blocks = [pl.ds(i, 16) for i in range(0, rows, 16)]
    for which in range(2):
        for sl in blocks:
            _, _, _, h = half(2, -1, which, sl)
            for c in range(3):
                hup_s[0, which, c, sl, :] = h[c][0].astype(BF16)
                hup_s[1, which, c, sl, :] = h[c][1].astype(BF16)
    send_up = pltpu.make_async_remote_copy(hup_s, hup_r, hsem.at[0], hsem.at[1], device_id=chip(n - 1), device_id_type=MESH)
    for which in range(2):
        for sl in blocks:
            _, _, _, h = half(2, 1, which, sl)
            h = colored(2, True, h)
            for c in range(3):
                hdn_s[0, which, c, sl, :] = h[c][0].astype(BF16)
                hdn_s[1, which, c, sl, :] = h[c][1].astype(BF16)
    send_dn = pltpu.make_async_remote_copy(hdn_s, hdn_r, hsem.at[2], hsem.at[3], device_id=chip(1), device_id_type=MESH)

    @pl.when(jnp.logical_not(down_later))
    def _():
        send_up.start()

    @pl.when(up_later)
    def _():
        pl.semaphore_wait(near_in.at[up], 1)

    send_dn.start()

    @pl.when(down_later)
    def _():
        pl.semaphore_wait(near_in.at[down], 1)
        send_up.start()

    tell(two_in.at[up], n - 1)
    tell(two_in.at[down], 1)
    load_b.wait()

    @pl.when(spin == 1)
    def _():
        pl.semaphore_wait(readyp, 1)

    swap_b = pltpu.make_async_remote_copy(bb.at[spin], bb.at[spin], bsem.at[0], bsem.at[1], device_id={"spin": 1 - spin}, device_id_type=MESH)
    swap_b.start()
    load_m.wait()
    sub = lax.broadcasted_iota(jnp.int32, (8, 128), 0)
    lane = lax.broadcasted_iota(jnp.int32, (8, 128), 1)
    x1, x2 = lane & (LX - 1), lane // LX
    width_y = 128 // LX

    def momentum(axis):
        value = jnp.full((8, 128), mom_ref[0, axis], jnp.int32)
        for p in range(1, nmom):
            value = jnp.where(sub == p, mom_ref[p, axis], value)
        return value

    turn = (((momentum(0) * x1) & (LX - 1)).astype(F32) / float(LX)
            + ((momentum(1) * x2) & (width_y - 1)).astype(F32) / float(width_y))
    turn = ((momentum(2) * z) & (n - 1)).astype(F32) / float(n) + turn
    theta = 2.0 * math.pi * turn
    cs[0] = jnp.cos(theta)
    cs[1] = jnp.sin(theta)

    first = lane[0:1, :] & (LX - 1)
    for mu in range(2):
        for which in range(2):
            for sl in blocks:
                for sign in (-1, 1):
                    s, t, beta, h = half(mu, sign, which, sl)
                    if sign == 1:
                        h = colored(mu, True, h)
                    moved = []
                    for pair in h:
                        if mu == 1:
                            moved.append(tuple(pltpu.roll(v, 128 - LX if sign == -1 else LX, 1) for v in pair))
                        elif sign == -1:
                            moved.append(tuple(jnp.where(first == LX - 1, pltpu.roll(v, LX - 1, 1), pltpu.roll(v, 127, 1)) for v in pair))
                        else:
                            moved.append(tuple(jnp.where(first == 0, pltpu.roll(v, 128 - (LX - 1), 1), pltpu.roll(v, 1, 1)) for v in pair))
                    h = moved
                    if sign == -1:
                        h = colored(mu, False, h)
                    for c in range(3):
                        other = times_unit(beta, h[c])
                        for ri in range(2):
                            if mu == 0 and sign == -1:
                                wv[ri, s, c, sl, :] = h[c][ri]
                                wv[ri, t, c, sl, :] = other[ri]
                            elif sign == -1:
                                wv[ri, s, c, sl, :] += h[c][ri]
                                wv[ri, t, c, sl, :] += other[ri]
                            else:
                                wv[ri, s, c, sl, :] -= h[c][ri]
                                wv[ri, t, c, sl, :] -= other[ri]

    load_t.wait()
    load_g.wait()
    half_rows = nmom * ngam * 2
    r = lax.broadcasted_iota(jnp.int32, (half_rows, 128), 0)
    l2 = lax.broadcasted_iota(jnp.int32, (half_rows, 128), 1)
    k_of = (r >> 1) & (ngam - 1)
    p_of = r // (2 * ngam)
    g_of = jnp.full((half_rows, 128), gam_ref[0], jnp.int32)
    for k in range(1, ngam):
        g_of = jnp.where(k_of == k, gam_ref[k], g_of)
    hot = jnp.where(l2 == g_of * (2 * nmom) + p_of * 2 + (r & 1), 1.0, 0.0).astype(BF16)
    for ri in range(2):
        lmat[pl.ds(ri * half_rows, half_rows), :] = jnp.dot(hot, tv[ri], preferred_element_type=F32).astype(BF16)

    swap_b.wait_recv()
    bf[...] = bb[...].astype(F32)
    for s in range(4):
        for which in range(2):
            for c in range(3):
                for a in range(2):
                    br = bf.at[which, 0, s, c][pl.ds(a, 16, stride=2), :]
                    bi = bf.at[which, 1, s, c][pl.ds(a, 16, stride=2), :]
                    for p in range(nmom):
                        co, si = cs[0, p:p + 1, :], cs[1, p:p + 1, :]
                        at_row = pl.ds((p * 4 + s) * 64 + a * 32 + which * 16, 16)
                        lh[at_row, pl.ds(c * 128, 128)] = (co * br - si * bi).astype(BF16)
                        lh[at_row, pl.ds((3 + c) * 128, 128)] = (si * br + co * bi).astype(BF16)

    send_up.wait_recv()
    for which in range(2):
        s, t, alpha, beta = projector(2, -1)[which]
        for sl in blocks:
            h = [(hup_r[0, which, c, sl, :].astype(F32), hup_r[1, which, c, sl, :].astype(F32)) for c in range(3)]
            h = colored(2, False, h)
            for c in range(3):
                other = times_unit(beta, h[c])
                for ri in range(2):
                    wv[ri, s, c, sl, :] += h[c][ri]
                    wv[ri, t, c, sl, :] += other[ri]
    send_dn.wait_recv()
    for which in range(2):
        s, t, alpha, beta = projector(2, 1)[which]
        for sl in blocks:
            start = sl.start
            for c in range(3):
                h = (hdn_r[0, which, c, sl, :].astype(F32), hdn_r[1, which, c, sl, :].astype(F32))
                other = times_unit(beta, h)
                for comp, value in ((s, h), (t, other)):
                    re = ((wv[0, comp, c, sl, :] - value[0]) * 0.5).astype(BF16)
                    im = ((wv[1, comp, c, sl, :] - value[1]) * 0.5).astype(BF16)
                    top, low = pl.ds(comp * rows + start, 16), pl.ds(4 * rows + comp * rows + start, 16)
                    rh[top, pl.ds(c * 128, 128)] = re
                    rh[top, pl.ds((3 + c) * 128, 128)] = im
                    rh[low, pl.ds(c * 128, 128)] = im
                    rh[low, pl.ds((3 + c) * 128, 128)] = -re

    for p in range(nmom):
        prod = lax.dot_general(lh[pl.ds(p * 256, 256), :], rh[...], (((1,), (1,)), ((), ())), preferred_element_type=F32)
        for j in range(8):
            for ri in range(2):
                rp[ri, pl.ds((p * 8 + j) * 40, 32), :] = prod[j * 32:(j + 1) * 32, ri * 128:(ri + 1) * 128]

    def partial(c):
        return [rp.at[ri][pl.ds(c, nmom * 8, stride=40), :] for ri in range(2)]

    centers = crole.shape[1]
    def part(side, m):
        forward_owner = lax.rem(z + jnp.where(side == 0, m, n - m), n)
        return jnp.concatenate(partial(forward_owner), axis=0)

    def post(side, steps, source, target, which):
        peer = {"space": lax.rem(z + jnp.where(side == 0, steps, n - steps), n)}
        return pltpu.make_async_remote_copy(source, target, csend.at[side, which], crecv.at[side, which], device_id=peer, device_id_type=MESH)

    def direct(side):
        return post(side, 1, c1.at[side, pl.ds(centers, 1)], r1.at[side, pl.ds(centers, 1)], 0)

    def near(side, i):
        return post(side, 1, c1.at[side, pl.ds(i, 1)], r1.at[side, pl.ds(i, 1)], 1 + i)

    def far(side, i):
        return post(side, 2, c2.at[side, pl.ds(i, 1)], r2.at[side, pl.ds(i, 1)], 1 + centers + i)

    def passed(side, i):
        to = centers - 1 if i == 0 else i - 1
        return post(side, 2 if i == 0 else STEP, crole.at[side, pl.ds(i, 1)], r3.at[side, pl.ds(to, 1)], 1 + 2 * centers + i)

    def has_far(side, i):
        m = STEP * i + 4
        return m < n // 2 or (m == n // 2 and side == up)

    levels = range(centers - 1, -1, -1)

    def center(side, i):
        total = part(side, STEP * i + 2)
        near(side, i).wait_recv()
        total = total + r1[side, i].astype(F32)
        if has_far(side, i):
            far(side, i).wait_recv()
            total = total + r2[side, i].astype(F32)
        if i < centers - 1:
            passed(side, i + 1).wait_recv()
            total = total + r3[side, i].astype(F32)
        crole[side, i] = total.astype(BF16)
        if i == centers - 1:
            pl.semaphore_wait(three_in.at[side], 1)
        passed(side, i).start()

    for side in range(2):
        c1[side, centers] = part(side, 1).astype(BF16)
        for i in levels:
            c1[side, i] = part(side, STEP * i + 3).astype(BF16)
            if has_far(side, i):
                c2[side, i] = part(side, STEP * i + 4).astype(BF16)
    for side in range(2):
        direct(side).start()
    for side in range(2):
        pl.semaphore_wait(two_in.at[side], 1)
        tell(three_in.at[side], n - 1 if side == up else 1)
        for i in levels:
            if has_far(side, i):
                far(side, i).start()
            near(side, i).start()
    def inside(i):
        return z >= STEP * (centers - 1 - i) + 7

    for i in levels:
        @pl.when(inside(i))
        def _():
            center(0, i)
    for i in levels:
        center(1, i)
    for i in levels:
        @pl.when(jnp.logical_not(inside(i)))
        def _():
            center(0, i)
    total = jnp.concatenate(partial(z), axis=0)
    for side in range(2):
        direct(side).wait_recv()
        passed(side, 0).wait_recv()
        total = total + r1[side, centers].astype(F32) + r3[side, centers - 1].astype(F32)
    stack = jnp.concatenate([total if s2 == 0 else pltpu.roll(total, 128 - s2 * rows, 1) for s2 in range(4)], axis=0)
    high = stack.astype(BF16)
    low = (stack - high.astype(F32)).astype(BF16)
    mat = lmat[:, 0:stack.shape[0]]
    out = jnp.dot(mat, high, preferred_element_type=F32) + jnp.dot(mat, low, preferred_element_type=F32)
    o_ref[...] = out[:, 0:rows] * scaling
    for side in range(2):
        direct(side).wait_send()
        for i in levels:
            near(side, i).wait_send()
            if has_far(side, i):
                far(side, i).wait_send()
            passed(side, i).wait_send()
    send_up.wait_send()
    send_dn.wait_send()
    swap_b.wait_send()


def solution(mesh):
    n = mesh.shape["space"]

    def body(backward, forward, gauge_links, momenta, gamma_list):
        cols, plane = forward.shape[3], forward.shape[6]
        nmom, ngam = momenta.shape[0], gamma_list.shape[0]
        scaling = 1.0 / math.sqrt(3.0 * plane * n)
        b = backward.transpose(0, 1, 2, 4, 5, 3, 6).reshape(2, 4, 3, cols, plane)
        f = forward.transpose(0, 1, 2, 4, 5, 3, 6).reshape(2, 4, 3, cols, plane)
        u = gauge_links.transpose(1, 2, 3, 4, 5, 0, 6).reshape(27, 2, plane)
        table = jnp.asarray(contraction_table(nmom), BF16)
        half_shape = (2, 2, 3, cols, plane)
        chunk = (nmom * 16, plane)
        n_rows = nmom * 4 * 2 * cols
        any_spec = pl.BlockSpec(memory_space=pl.ANY)
        centers = (n // 2 - 2) // STEP + 1
        out = pl.pallas_call(
            functools.partial(kernel, n, nmom, ngam, scaling),
            out_shape=jax.ShapeDtypeStruct((2 * nmom * ngam * 2, cols), F32),
            in_specs=[any_spec, any_spec, any_spec, any_spec, any_spec, any_spec],
            out_specs=pl.BlockSpec(memory_space=pltpu.VMEM),
            name="insertion",
            scratch_shapes=[
                pltpu.VMEM(f.shape, BF16),
                pltpu.VMEM(u.shape, BF16),
                pltpu.VMEM(table.shape, BF16),
                pltpu.VMEM((2, *b.shape), BF16),
                pltpu.VMEM(f.shape, F32),
                pltpu.VMEM(u.shape, F32),
                pltpu.VMEM((2, *b.shape), F32),
                pltpu.VMEM(f.shape, F32),
                pltpu.VMEM((n_rows, 6 * plane), BF16),
                pltpu.VMEM((8 * cols, 6 * plane), BF16),
                pltpu.VMEM((2, nmom * 8 * 40, plane), F32),
                pltpu.VMEM(half_shape, BF16),
                pltpu.VMEM(half_shape, BF16),
                pltpu.VMEM(half_shape, BF16),
                pltpu.VMEM(half_shape, BF16),
                pltpu.VMEM((2, centers + 1, *chunk), BF16),
                pltpu.VMEM((2, centers, *chunk), BF16),
                pltpu.VMEM((2, centers, *chunk), BF16),
                pltpu.VMEM((2, centers + 1, *chunk), BF16),
                pltpu.VMEM((2, centers, *chunk), BF16),
                pltpu.VMEM((2, centers, *chunk), BF16),
                pltpu.VMEM((2, 8, plane), F32),
                pltpu.VMEM((2 * nmom * ngam * 2, 256), BF16),
                pltpu.SMEM(momenta.shape, jnp.int32),
                pltpu.SMEM(gamma_list.shape, jnp.int32),
                pltpu.SemaphoreType.DMA((6,)),
                pltpu.SemaphoreType.DMA((2,)),
                pltpu.SemaphoreType.DMA((4,)),
                pltpu.SemaphoreType.DMA((2, 1 + 3 * centers)),
                pltpu.SemaphoreType.DMA((2, 1 + 3 * centers)),
                pltpu.SemaphoreType.REGULAR((3, 2)),
                pltpu.SemaphoreType.REGULAR,
            ],
            compiler_params=pltpu.CompilerParams(collective_id=0, has_side_effects=True, vmem_limit_bytes=67043328),
        )(momenta, gamma_list, b, f, u, table)
        return out.reshape(2, nmom, ngam, 1, 2, cols)

    in_specs = (
        P("parts", "tm", None, "spin", None, "space", None),
        P("parts", "tm", None, "spin", None, "space", None),
        P("parts", None, None, None, "tm", "space", None),
        P(),
        P(),
    )
    out_specs = P("parts", None, None, "tm", "space", "spin")
    return jax.shard_map(body, mesh=mesh, in_specs=in_specs, out_specs=out_specs, check_vma=False)
```

```python
import functools
import math

import jax
import jax.numpy as jnp
import numpy as np
from jax import lax
from jax.experimental import pallas as pl
from jax.experimental.pallas import tpu as pltpu
from jax.sharding import PartitionSpec as P

MESH = pl.DeviceIdType.MESH
LX = 32
F32 = jnp.float32
BF16 = jnp.bfloat16

STEP = 3
REACH = STEP + 2


def gamma_tables():
    zeros = np.zeros((4, 4))
    gx = np.array([[0, 0, 0, 1j], [0, 0, 1j, 0], [0, -1j, 0, 0], [-1j, 0, 0, 0]])
    gy = np.array([[0, 0, 0, -1], [0, 0, 1, 0], [0, 1, 0, 0], [-1, 0, 0, 0]]) + 0j
    gz = np.array([[0, 0, 1j, 0], [0, 0, 0, -1j], [-1j, 0, 0, 0], [0, 1j, 0, 0]])
    gt = np.array([[0, 0, 1, 0], [0, 0, 0, 1], [1, 0, 0, 0], [0, 1, 0, 0]]) + 0j
    singles = [gx, gy, gz, gt]
    basis = []
    for number in range(16):
        mat = np.eye(4) + 0j
        for which in range(4):
            if number >> which & 1:
                mat = mat @ singles[which]
        basis.append(mat)
    return singles, np.stack(basis)


def contraction_table(nmom):
    _, basis = gamma_tables()
    table = np.zeros((2, 128, 256), np.float32)
    for g in range(16):
        for p in range(nmom):
            for a in range(2):
                row = g * 2 * nmom + p * 2 + a
                for s in range(4):
                    for s2 in range(4):
                        value = basis[g][s, s2]
                        for ri_out, ri_in, coef in ((0, 0, value.real), (0, 1, -value.imag), (1, 0, value.imag), (1, 1, value.real)):
                            table[ri_out, row, ((s2 * 2 + ri_in) * nmom + p) * 8 + s * 2 + a] = coef
    return table


def times_unit(coef, value):
    re, im = value
    if coef == 1:
        return re, im
    if coef == -1:
        return -re, -im
    if coef == 1j:
        return -im, re
    assert coef == -1j
    return im, -re


def plus(x, y):
    return x[0] + y[0], x[1] + y[1]


def projector(mu, sign):
    singles, _ = gamma_tables()
    mat = np.eye(4) + sign * singles[mu]
    result = []
    for s in range(2):
        t = [t for t in (2, 3) if mat[s, t] != 0][0]
        result.append((s, t, complex(mat[s, t]), complex(mat[t, s])))
    return result


def kernel(n, nmom, ngam, scaling,
           mom_hbm, gam_hbm, b_hbm, f_hbm, u_hbm, t_hbm, o_ref,
           fv, uv, tv, bb, ff, uf, bf, wv, lh, rh, rp, hup_s, hup_r, hdn_s, hdn_r, c1, c2, crole, r1, r2, r3, cs, lmat, mom_ref, gam_ref,
           lsem, bsem, hsem, csend, crecv, inside_sem, readyp):
    z = lax.axis_index("space")
    spin = lax.axis_index("spin")
    rows = fv.shape[3]

    load_f = pltpu.make_async_copy(f_hbm, fv, lsem.at[0])
    load_u = pltpu.make_async_copy(u_hbm, uv, lsem.at[1])
    load_b = pltpu.make_async_copy(b_hbm, bb.at[spin], lsem.at[2])
    load_t = pltpu.make_async_copy(t_hbm, tv, lsem.at[3])
    load_m = pltpu.make_async_copy(mom_hbm, mom_ref, lsem.at[4])
    load_g = pltpu.make_async_copy(gam_hbm, gam_ref, lsem.at[5])
    for copy in (load_f, load_u, load_b, load_t, load_m, load_g):
        copy.start()

    def chip(d):
        return {"space": lax.rem(z + d, n)}

    def tell(sem, d):
        pl.semaphore_signal(sem, inc=1, device_id=chip(d), device_id_type=MESH)

    up, down = 0, 1
    last = z == n - 1
    near_in, two_in = inside_sem.at[0], inside_sem.at[1]
    barrier = pltpu.get_barrier_semaphore()
    def hear(side, distance):
        pl.semaphore_wait(inside_sem.at[distance - 1, side], 1)
        if distance < REACH:
            tell(inside_sem.at[distance, side], n - 1 if side == up else 1)

    up_later = jnp.logical_and(z > 0, jnp.logical_not(last))
    down_later = z < 2

    @pl.when(up_later)
    def _():
        tell(barrier, 1)

    @pl.when(down_later)
    def _():
        tell(barrier, n - 1)

    @pl.when(spin == 1)
    def _():
        pl.semaphore_signal(barrier, inc=1, device_id={"spin": 0}, device_id_type=MESH)

    count = jnp.where(up_later, 0, 1) + jnp.where(down_later, 0, 1) + jnp.where(spin == 0, 1, 0)

    @pl.when(count > 0)
    def _():
        pl.semaphore_wait(barrier, count)

    @pl.when(jnp.logical_not(down_later))
    def _():
        tell(near_in.at[up], n - 1)

    @pl.when(jnp.logical_not(up_later))
    def _():
        tell(near_in.at[down], 1)

    @pl.when(spin == 0)
    def _():
        pl.semaphore_signal(readyp, inc=1, device_id={"spin": 1}, device_id_type=MESH)

    load_f.wait()
    load_u.wait()
    ff[...] = fv[...].astype(F32)
    for i in range(uv.shape[0]):
        uf[i] = uv[i].astype(F32)

    def link(mu, c, d, dagger):
        if dagger:
            return uf[mu * 9 + d * 3 + c, 0:1, :], -uf[mu * 9 + d * 3 + c, 1:2, :]
        return uf[mu * 9 + c * 3 + d, 0:1, :], uf[mu * 9 + c * 3 + d, 1:2, :]

    def colored(mu, dagger, h):
        out = []
        for c in range(3):
            re = im = None
            for d in range(3):
                cr, ci = link(mu, c, d, dagger)
                hr, hi = h[d]
                pr, pi = cr * hr - ci * hi, cr * hi + ci * hr
                re, im = (pr, pi) if re is None else (re + pr, im + pi)
            out.append((re, im))
        return out

    def half(mu, sign, which, sl):
        s, t, alpha, beta = projector(mu, sign)[which]
        h = []
        for c in range(3):
            x = (ff[0, s, c, sl, :], ff[1, s, c, sl, :])
            y = (ff[0, t, c, sl, :], ff[1, t, c, sl, :])
            h.append(plus(x, times_unit(alpha, y)))
        return s, t, beta, h

    blocks = [pl.ds(i, 16) for i in range(0, rows, 16)]
    for which in range(2):
        for sl in blocks:
            _, _, _, h = half(2, -1, which, sl)
            for c in range(3):
                hup_s[0, which, c, sl, :] = h[c][0].astype(BF16)
                hup_s[1, which, c, sl, :] = h[c][1].astype(BF16)
    send_up = pltpu.make_async_remote_copy(hup_s, hup_r, hsem.at[0], hsem.at[1], device_id=chip(n - 1), device_id_type=MESH)
    for which in range(2):
        for sl in blocks:
            _, _, _, h = half(2, 1, which, sl)
            h = colored(2, True, h)
            for c in range(3):
                hdn_s[0, which, c, sl, :] = h[c][0].astype(BF16)
                hdn_s[1, which, c, sl, :] = h[c][1].astype(BF16)
    send_dn = pltpu.make_async_remote_copy(hdn_s, hdn_r, hsem.at[2], hsem.at[3], device_id=chip(1), device_id_type=MESH)

    @pl.when(jnp.logical_not(down_later))
    def _():
        send_up.start()

    @pl.when(up_later)
    def _():
        pl.semaphore_wait(near_in.at[up], 1)

    send_dn.start()

    @pl.when(down_later)
    def _():
        pl.semaphore_wait(near_in.at[down], 1)
        send_up.start()

    tell(two_in.at[up], n - 1)
    tell(two_in.at[down], 1)
    load_b.wait()

    @pl.when(spin == 1)
    def _():
        pl.semaphore_wait(readyp, 1)

    swap_b = pltpu.make_async_remote_copy(bb.at[spin], bb.at[spin], bsem.at[0], bsem.at[1], device_id={"spin": 1 - spin}, device_id_type=MESH)
    swap_b.start()
    load_m.wait()
    sub = lax.broadcasted_iota(jnp.int32, (8, 128), 0)
    lane = lax.broadcasted_iota(jnp.int32, (8, 128), 1)
    x1, x2 = lane & (LX - 1), lane // LX
    width_y = 128 // LX

    def momentum(axis):
        value = jnp.full((8, 128), mom_ref[0, axis], jnp.int32)
        for p in range(1, nmom):
            value = jnp.where(sub == p, mom_ref[p, axis], value)
        return value

    turn = (((momentum(0) * x1) & (LX - 1)).astype(F32) / float(LX)
            + ((momentum(1) * x2) & (width_y - 1)).astype(F32) / float(width_y))
    turn = ((momentum(2) * z) & (n - 1)).astype(F32) / float(n) + turn
    theta = 2.0 * math.pi * turn
    cs[0] = jnp.cos(theta)
    cs[1] = jnp.sin(theta)

    first = lane[0:1, :] & (LX - 1)
    for mu in range(2):
        for which in range(2):
            for sl in blocks:
                for sign in (-1, 1):
                    s, t, beta, h = half(mu, sign, which, sl)
                    if sign == 1:
                        h = colored(mu, True, h)
                    moved = []
                    for pair in h:
                        if mu == 1:
                            moved.append(tuple(pltpu.roll(v, 128 - LX if sign == -1 else LX, 1) for v in pair))
                        elif sign == -1:
                            moved.append(tuple(jnp.where(first == LX - 1, pltpu.roll(v, LX - 1, 1), pltpu.roll(v, 127, 1)) for v in pair))
                        else:
                            moved.append(tuple(jnp.where(first == 0, pltpu.roll(v, 128 - (LX - 1), 1), pltpu.roll(v, 1, 1)) for v in pair))
                    h = moved
                    if sign == -1:
                        h = colored(mu, False, h)
                    for c in range(3):
                        other = times_unit(beta, h[c])
                        for ri in range(2):
                            if mu == 0 and sign == -1:
                                wv[ri, s, c, sl, :] = h[c][ri]
                                wv[ri, t, c, sl, :] = other[ri]
                            elif sign == -1:
                                wv[ri, s, c, sl, :] += h[c][ri]
                                wv[ri, t, c, sl, :] += other[ri]
                            else:
                                wv[ri, s, c, sl, :] -= h[c][ri]
                                wv[ri, t, c, sl, :] -= other[ri]

    load_t.wait()
    load_g.wait()
    half_rows = nmom * ngam * 2
    r = lax.broadcasted_iota(jnp.int32, (half_rows, 128), 0)
    l2 = lax.broadcasted_iota(jnp.int32, (half_rows, 128), 1)
    k_of = (r >> 1) & (ngam - 1)
    p_of = r // (2 * ngam)
    g_of = jnp.full((half_rows, 128), gam_ref[0], jnp.int32)
    for k in range(1, ngam):
        g_of = jnp.where(k_of == k, gam_ref[k], g_of)
    hot = jnp.where(l2 == g_of * (2 * nmom) + p_of * 2 + (r & 1), 1.0, 0.0).astype(BF16)
    for ri in range(2):
        lmat[pl.ds(ri * half_rows, half_rows), :] = jnp.dot(hot, tv[ri], preferred_element_type=F32).astype(BF16)

    swap_b.wait_recv()
    bf[...] = bb[...].astype(F32)
    for s in range(4):
        for which in range(2):
            for c in range(3):
                for a in range(2):
                    br = bf.at[which, 0, s, c][pl.ds(a, 16, stride=2), :]
                    bi = bf.at[which, 1, s, c][pl.ds(a, 16, stride=2), :]
                    for p in range(nmom):
                        co, si = cs[0, p:p + 1, :], cs[1, p:p + 1, :]
                        at_row = pl.ds((p * 4 + s) * 64 + a * 32 + which * 16, 16)
                        lh[at_row, pl.ds(c * 128, 128)] = (co * br - si * bi).astype(BF16)
                        lh[at_row, pl.ds((3 + c) * 128, 128)] = (si * br + co * bi).astype(BF16)

    for distance in range(2, REACH + 1):
        @pl.when(z > distance)
        def _():
            hear(down, distance)
    hear(up, 2)
    send_up.wait_recv()
    for which in range(2):
        s, t, alpha, beta = projector(2, -1)[which]
        for sl in blocks:
            h = [(hup_r[0, which, c, sl, :].astype(F32), hup_r[1, which, c, sl, :].astype(F32)) for c in range(3)]
            h = colored(2, False, h)
            for c in range(3):
                other = times_unit(beta, h[c])
                for ri in range(2):
                    wv[ri, s, c, sl, :] += h[c][ri]
                    wv[ri, t, c, sl, :] += other[ri]
    send_dn.wait_recv()
    for which in range(2):
        s, t, alpha, beta = projector(2, 1)[which]
        for sl in blocks:
            start = sl.start
            for c in range(3):
                h = (hdn_r[0, which, c, sl, :].astype(F32), hdn_r[1, which, c, sl, :].astype(F32))
                other = times_unit(beta, h)
                for comp, value in ((s, h), (t, other)):
                    re = ((wv[0, comp, c, sl, :] - value[0]) * 0.5).astype(BF16)
                    im = ((wv[1, comp, c, sl, :] - value[1]) * 0.5).astype(BF16)
                    top, low = pl.ds(comp * rows + start, 16), pl.ds(4 * rows + comp * rows + start, 16)
                    rh[top, pl.ds(c * 128, 128)] = re
                    rh[top, pl.ds((3 + c) * 128, 128)] = im
                    rh[low, pl.ds(c * 128, 128)] = im
                    rh[low, pl.ds((3 + c) * 128, 128)] = -re

    for p in range(nmom):
        prod = lax.dot_general(lh[pl.ds(p * 256, 256), :], rh[...], (((1,), (1,)), ((), ())), preferred_element_type=F32)
        for j in range(8):
            for ri in range(2):
                rp[ri, pl.ds((p * 8 + j) * 40, 32), :] = prod[j * 32:(j + 1) * 32, ri * 128:(ri + 1) * 128]

    def partial(c):
        return [rp.at[ri][pl.ds(c, nmom * 8, stride=40), :] for ri in range(2)]

    centers = crole.shape[1]
    def part(side, m):
        forward_owner = lax.rem(z + jnp.where(side == 0, m, n - m), n)
        return jnp.concatenate(partial(forward_owner), axis=0)

    def post(side, steps, source, target, which):
        peer = {"space": lax.rem(z + jnp.where(side == 0, steps, n - steps), n)}
        return pltpu.make_async_remote_copy(source, target, csend.at[side, which], crecv.at[side, which], device_id=peer, device_id_type=MESH)

    def direct(side):
        return post(side, 1, c1.at[side, pl.ds(centers, 1)], r1.at[side, pl.ds(centers, 1)], 0)

    def near(side, i):
        return post(side, 1, c1.at[side, pl.ds(i, 1)], r1.at[side, pl.ds(i, 1)], 1 + i)

    def far(side, i):
        return post(side, 2, c2.at[side, pl.ds(i, 1)], r2.at[side, pl.ds(i, 1)], 1 + centers + i)

    def passed(side, i):
        to = (0, centers - 1)[i] if i < 2 else i - 1
        steps = STEP * i + 2 if i < 2 else STEP
        return post(side, steps, crole.at[side, pl.ds(i, 1)], r3.at[side, pl.ds(to, 1)], 1 + 2 * centers + i)

    def has_far(side, i):
        m = STEP * i + 4
        return m < n // 2 or (m == n // 2 and side == up)

    levels = range(centers - 1, -1, -1)

    def center(side, i):
        total = part(side, STEP * i + 2)
        near(side, i).wait_recv()
        total = total + r1[side, i].astype(F32)
        if has_far(side, i):
            far(side, i).wait_recv()
            total = total + r2[side, i].astype(F32)
        if 0 < i < centers - 1:
            passed(side, i + 1).wait_recv()
            total = total + r3[side, i].astype(F32)
        crole[side, i] = total.astype(BF16)
        passed(side, i).start()

    for side in range(2):
        c1[side, centers] = part(side, 1).astype(BF16)
        for i in levels:
            c1[side, i] = part(side, STEP * i + 3).astype(BF16)
            if has_far(side, i):
                c2[side, i] = part(side, STEP * i + 4).astype(BF16)
    def hear_late(distance):
        @pl.when(z <= distance)
        def _():
            hear(down, distance)

    for side in range(2):
        direct(side).start()
    for side in range(2):
        if side == down:
            hear_late(2)
        for i in levels:
            if has_far(side, i):
                far(side, i).start()
            near(side, i).start()
    hear(up, 3)
    def inside(i):
        return z >= STEP * (centers - 1 - i if i else 0) + 7

    order = [i for i in levels if i > 1] + [0]

    def inner(i):
        @pl.when(inside(i))
        def _():
            center(up, i)

    for i in order:
        inner(i)
        if i == centers - 1:
            hear(up, 4)
    hear(up, REACH)
    inner(1)
    center(down, 0)
    hear_late(3)
    for i in order[:-1]:
        center(down, i)
    for distance in range(4, REACH + 1):
        hear_late(distance)
    center(down, 1)
    for i in [*order, 1]:
        @pl.when(jnp.logical_not(inside(i)))
        def _():
            center(up, i)
    total = jnp.concatenate(partial(z), axis=0)
    for side in range(2):
        direct(side).wait_recv()
        passed(side, 0).wait_recv()
        passed(side, 1).wait_recv()
        total = total + r1[side, centers].astype(F32) + r3[side, 0].astype(F32) + r3[side, centers - 1].astype(F32)
    stack = jnp.concatenate([total if s2 == 0 else pltpu.roll(total, 128 - s2 * rows, 1) for s2 in range(4)], axis=0)
    high = stack.astype(BF16)
    low = (stack - high.astype(F32)).astype(BF16)
    mat = lmat[:, 0:stack.shape[0]]
    out = jnp.dot(mat, high, preferred_element_type=F32) + jnp.dot(mat, low, preferred_element_type=F32)
    o_ref[...] = out[:, 0:rows] * scaling
    for side in range(2):
        direct(side).wait_send()
        for i in levels:
            near(side, i).wait_send()
            if has_far(side, i):
                far(side, i).wait_send()
            passed(side, i).wait_send()
    send_up.wait_send()
    send_dn.wait_send()
    swap_b.wait_send()


def solution(mesh):
    n = mesh.shape["space"]

    def body(backward, forward, gauge_links, momenta, gamma_list):
        cols, plane = forward.shape[3], forward.shape[6]
        nmom, ngam = momenta.shape[0], gamma_list.shape[0]
        scaling = 1.0 / math.sqrt(3.0 * plane * n)
        b = backward.transpose(0, 1, 2, 4, 5, 3, 6).reshape(2, 4, 3, cols, plane)
        f = forward.transpose(0, 1, 2, 4, 5, 3, 6).reshape(2, 4, 3, cols, plane)
        u = gauge_links.transpose(1, 2, 3, 4, 5, 0, 6).reshape(27, 2, plane)
        table = jnp.asarray(contraction_table(nmom), BF16)
        half_shape = (2, 2, 3, cols, plane)
        chunk = (nmom * 16, plane)
        n_rows = nmom * 4 * 2 * cols
        any_spec = pl.BlockSpec(memory_space=pltpu.MemorySpace.HBM)
        centers = (n // 2 - 2) // STEP + 1
        out = pl.pallas_call(
            functools.partial(kernel, n, nmom, ngam, scaling),
            out_shape=jax.ShapeDtypeStruct((2 * nmom * ngam * 2, cols), F32),
            in_specs=[any_spec, any_spec, any_spec, any_spec, any_spec, any_spec],
            out_specs=pl.BlockSpec(memory_space=pltpu.VMEM),
            name="insertion",
            scratch_shapes=[
                pltpu.VMEM(f.shape, BF16),
                pltpu.VMEM(u.shape, BF16),
                pltpu.VMEM(table.shape, BF16),
                pltpu.VMEM((2, *b.shape), BF16),
                pltpu.VMEM(f.shape, F32),
                pltpu.VMEM(u.shape, F32),
                pltpu.VMEM((2, *b.shape), F32),
                pltpu.VMEM(f.shape, F32),
                pltpu.VMEM((n_rows, 6 * plane), BF16),
                pltpu.VMEM((8 * cols, 6 * plane), BF16),
                pltpu.VMEM((2, nmom * 8 * 40, plane), F32),
                pltpu.VMEM(half_shape, BF16),
                pltpu.VMEM(half_shape, BF16),
                pltpu.VMEM(half_shape, BF16),
                pltpu.VMEM(half_shape, BF16),
                pltpu.VMEM((2, centers + 1, *chunk), BF16),
                pltpu.VMEM((2, centers, *chunk), BF16),
                pltpu.VMEM((2, centers, *chunk), BF16),
                pltpu.VMEM((2, centers + 1, *chunk), BF16),
                pltpu.VMEM((2, centers, *chunk), BF16),
                pltpu.VMEM((2, centers, *chunk), BF16),
                pltpu.VMEM((2, 8, plane), F32),
                pltpu.VMEM((2 * nmom * ngam * 2, 256), BF16),
                pltpu.SMEM(momenta.shape, jnp.int32),
                pltpu.SMEM(gamma_list.shape, jnp.int32),
                pltpu.SemaphoreType.DMA((6,)),
                pltpu.SemaphoreType.DMA((2,)),
                pltpu.SemaphoreType.DMA((4,)),
                pltpu.SemaphoreType.DMA((2, 1 + 3 * centers)),
                pltpu.SemaphoreType.DMA((2, 1 + 3 * centers)),
                pltpu.SemaphoreType.REGULAR((REACH, 2)),
                pltpu.SemaphoreType.REGULAR,
            ],
            compiler_params=pltpu.CompilerParams(collective_id=0, has_side_effects=True, vmem_limit_bytes=40 * 2**20),
        )(*[pltpu.with_memory_space_constraint(v, pltpu.MemorySpace.HBM) for v in (momenta, gamma_list, b, f, u, table)])
        return out.reshape(2, nmom, ngam, 1, 2, cols)

    in_specs = (
        P("parts", "tm", None, "spin", None, "space", None),
        P("parts", "tm", None, "spin", None, "space", None),
        P("parts", None, None, None, "tm", "space", None),
        P(),
        P(),
    )
    out_specs = P("parts", None, None, "tm", "space", "spin")
    return jax.shard_map(body, mesh=mesh, in_specs=in_specs, out_specs=out_specs, check_vma=False)
```

```python
import functools
import math

import jax
import jax.numpy as jnp
import numpy as np
from jax import lax
from jax.experimental import pallas as pl
from jax.experimental.pallas import tpu as pltpu
from jax.sharding import PartitionSpec as P

MESH = pl.DeviceIdType.MESH
LX = 32
F32 = jnp.float32
BF16 = jnp.bfloat16

STEP = 3
REACH = STEP + 2


def gamma_tables():
    zeros = np.zeros((4, 4))
    gx = np.array([[0, 0, 0, 1j], [0, 0, 1j, 0], [0, -1j, 0, 0], [-1j, 0, 0, 0]])
    gy = np.array([[0, 0, 0, -1], [0, 0, 1, 0], [0, 1, 0, 0], [-1, 0, 0, 0]]) + 0j
    gz = np.array([[0, 0, 1j, 0], [0, 0, 0, -1j], [-1j, 0, 0, 0], [0, 1j, 0, 0]])
    gt = np.array([[0, 0, 1, 0], [0, 0, 0, 1], [1, 0, 0, 0], [0, 1, 0, 0]]) + 0j
    singles = [gx, gy, gz, gt]
    basis = []
    for number in range(16):
        mat = np.eye(4) + 0j
        for which in range(4):
            if number >> which & 1:
                mat = mat @ singles[which]
        basis.append(mat)
    return singles, np.stack(basis)


def contraction_table(nmom):
    _, basis = gamma_tables()
    table = np.zeros((2, 128, 256), np.float32)
    for g in range(16):
        for p in range(nmom):
            for a in range(2):
                row = g * 2 * nmom + p * 2 + a
                for s in range(4):
                    for s2 in range(4):
                        value = basis[g][s, s2]
                        for ri_out, ri_in, coef in ((0, 0, value.real), (0, 1, -value.imag), (1, 0, value.imag), (1, 1, value.real)):
                            table[ri_out, row, ((s2 * 2 + ri_in) * nmom + p) * 8 + s * 2 + a] = coef
    return table


def times_unit(coef, value):
    re, im = value
    if coef == 1:
        return re, im
    if coef == -1:
        return -re, -im
    if coef == 1j:
        return -im, re
    assert coef == -1j
    return im, -re


def plus(x, y):
    return x[0] + y[0], x[1] + y[1]


def projector(mu, sign):
    singles, _ = gamma_tables()
    mat = np.eye(4) + sign * singles[mu]
    result = []
    for s in range(2):
        t = [t for t in (2, 3) if mat[s, t] != 0][0]
        result.append((s, t, complex(mat[s, t]), complex(mat[t, s])))
    return result


def kernel(n, nmom, ngam, scaling,
           mom_hbm, gam_hbm, b_hbm, f_hbm, u_hbm, t_hbm, o_ref,
           fv, uv, tv, bb, ff, uf, bf, wv, lh, rh, rp, hup_s, hup_r, hdn_s, hdn_r, c1, c2, crole, r1, r2, r3, cs, lmat, mom_ref, gam_ref,
           lsem, bsem, hsem, csend, crecv, inside_sem, readyp):
    z = lax.axis_index("space")
    spin = lax.axis_index("spin")
    rows = fv.shape[3]

    load_f = pltpu.make_async_copy(f_hbm, fv, lsem.at[0])
    load_u = pltpu.make_async_copy(u_hbm, uv, lsem.at[1])
    load_b = pltpu.make_async_copy(b_hbm, bb.at[spin], lsem.at[2])
    load_t = pltpu.make_async_copy(t_hbm, tv, lsem.at[3])
    load_m = pltpu.make_async_copy(mom_hbm, mom_ref, lsem.at[4])
    load_g = pltpu.make_async_copy(gam_hbm, gam_ref, lsem.at[5])
    for copy in (load_f, load_u, load_b, load_t, load_m, load_g):
        copy.start()

    def chip(d):
        return {"space": lax.rem(z + d, n)}

    def tell(sem, d):
        pl.semaphore_signal(sem, inc=1, device_id=chip(d), device_id_type=MESH)

    up, down = 0, 1
    last = z == n - 1
    near_in, two_in = inside_sem.at[0], inside_sem.at[1]
    barrier = pltpu.get_barrier_semaphore()
    def hear(side, distance):
        pl.semaphore_wait(inside_sem.at[distance - 1, side], 1)
        if distance < REACH:
            tell(inside_sem.at[distance, side], n - 1 if side == up else 1)

    up_later = jnp.logical_and(z > 0, jnp.logical_not(last))
    down_later = z < 2

    @pl.when(up_later)
    def _():
        tell(barrier, 1)

    @pl.when(down_later)
    def _():
        tell(barrier, n - 1)

    @pl.when(spin == 1)
    def _():
        pl.semaphore_signal(barrier, inc=1, device_id={"spin": 0}, device_id_type=MESH)

    count = jnp.where(up_later, 0, 1) + jnp.where(down_later, 0, 1) + jnp.where(spin == 0, 1, 0)

    @pl.when(count > 0)
    def _():
        pl.semaphore_wait(barrier, count)

    @pl.when(jnp.logical_not(down_later))
    def _():
        tell(near_in.at[up], n - 1)

    @pl.when(jnp.logical_not(up_later))
    def _():
        tell(near_in.at[down], 1)

    @pl.when(spin == 0)
    def _():
        pl.semaphore_signal(readyp, inc=1, device_id={"spin": 1}, device_id_type=MESH)

    load_f.wait()
    load_u.wait()
    ff[...] = fv[...].astype(F32)
    for i in range(uv.shape[0]):
        uf[i] = uv[i].astype(F32)

    def link(mu, c, d, dagger):
        if dagger:
            return uf[mu * 9 + d * 3 + c, 0:1, :], -uf[mu * 9 + d * 3 + c, 1:2, :]
        return uf[mu * 9 + c * 3 + d, 0:1, :], uf[mu * 9 + c * 3 + d, 1:2, :]

    def colored(mu, dagger, h):
        out = []
        for c in range(3):
            re = im = None
            for d in range(3):
                cr, ci = link(mu, c, d, dagger)
                hr, hi = h[d]
                pr, pi = cr * hr - ci * hi, cr * hi + ci * hr
                re, im = (pr, pi) if re is None else (re + pr, im + pi)
            out.append((re, im))
        return out

    def half(mu, sign, which, sl):
        s, t, alpha, beta = projector(mu, sign)[which]
        h = []
        for c in range(3):
            x = (ff[0, s, c, sl, :], ff[1, s, c, sl, :])
            y = (ff[0, t, c, sl, :], ff[1, t, c, sl, :])
            h.append(plus(x, times_unit(alpha, y)))
        return s, t, beta, h

    blocks = [pl.ds(i, 16) for i in range(0, rows, 16)]
    for which in range(2):
        for sl in blocks:
            _, _, _, h = half(2, -1, which, sl)
            for c in range(3):
                hup_s[0, which, c, sl, :] = h[c][0].astype(BF16)
                hup_s[1, which, c, sl, :] = h[c][1].astype(BF16)
    send_up = pltpu.make_async_remote_copy(hup_s, hup_r, hsem.at[0], hsem.at[1], device_id=chip(n - 1), device_id_type=MESH)
    for which in range(2):
        for sl in blocks:
            _, _, _, h = half(2, 1, which, sl)
            h = colored(2, True, h)
            for c in range(3):
                hdn_s[0, which, c, sl, :] = h[c][0].astype(BF16)
                hdn_s[1, which, c, sl, :] = h[c][1].astype(BF16)
    send_dn = pltpu.make_async_remote_copy(hdn_s, hdn_r, hsem.at[2], hsem.at[3], device_id=chip(1), device_id_type=MESH)

    @pl.when(jnp.logical_not(down_later))
    def _():
        send_up.start()

    @pl.when(up_later)
    def _():
        pl.semaphore_wait(near_in.at[up], 1)

    send_dn.start()

    @pl.when(down_later)
    def _():
        pl.semaphore_wait(near_in.at[down], 1)
        send_up.start()

    tell(two_in.at[up], n - 1)
    tell(two_in.at[down], 1)
    load_b.wait()

    @pl.when(spin == 1)
    def _():
        pl.semaphore_wait(readyp, 1)

    swap_b = pltpu.make_async_remote_copy(bb.at[spin], bb.at[spin], bsem.at[0], bsem.at[1], device_id={"spin": 1 - spin}, device_id_type=MESH)
    swap_b.start()
    load_m.wait()
    sub = lax.broadcasted_iota(jnp.int32, (8, 128), 0)
    lane = lax.broadcasted_iota(jnp.int32, (8, 128), 1)
    x1, x2 = lane & (LX - 1), lane // LX
    width_y = 128 // LX

    def momentum(axis):
        value = jnp.full((8, 128), mom_ref[0, axis], jnp.int32)
        for p in range(1, nmom):
            value = jnp.where(sub == p, mom_ref[p, axis], value)
        return value

    turn = (((momentum(0) * x1) & (LX - 1)).astype(F32) / float(LX)
            + ((momentum(1) * x2) & (width_y - 1)).astype(F32) / float(width_y))
    turn = ((momentum(2) * z) & (n - 1)).astype(F32) / float(n) + turn
    theta = 2.0 * math.pi * turn
    cs[0] = jnp.cos(theta)
    cs[1] = jnp.sin(theta)

    first = lane[0:1, :] & (LX - 1)
    for mu in range(2):
        for which in range(2):
            for sl in blocks:
                for sign in (-1, 1):
                    s, t, beta, h = half(mu, sign, which, sl)
                    if sign == 1:
                        h = colored(mu, True, h)
                    moved = []
                    for pair in h:
                        if mu == 1:
                            moved.append(tuple(pltpu.roll(v, 128 - LX if sign == -1 else LX, 1) for v in pair))
                        elif sign == -1:
                            moved.append(tuple(jnp.where(first == LX - 1, pltpu.roll(v, LX - 1, 1), pltpu.roll(v, 127, 1)) for v in pair))
                        else:
                            moved.append(tuple(jnp.where(first == 0, pltpu.roll(v, 128 - (LX - 1), 1), pltpu.roll(v, 1, 1)) for v in pair))
                    h = moved
                    if sign == -1:
                        h = colored(mu, False, h)
                    for c in range(3):
                        other = times_unit(beta, h[c])
                        for ri in range(2):
                            if mu == 0 and sign == -1:
                                wv[ri, s, c, sl, :] = h[c][ri]
                                wv[ri, t, c, sl, :] = other[ri]
                            elif sign == -1:
                                wv[ri, s, c, sl, :] += h[c][ri]
                                wv[ri, t, c, sl, :] += other[ri]
                            else:
                                wv[ri, s, c, sl, :] -= h[c][ri]
                                wv[ri, t, c, sl, :] -= other[ri]

    load_t.wait()
    load_g.wait()
    half_rows = nmom * ngam * 2
    r = lax.broadcasted_iota(jnp.int32, (half_rows, 128), 0)
    l2 = lax.broadcasted_iota(jnp.int32, (half_rows, 128), 1)
    k_of = (r >> 1) & (ngam - 1)
    p_of = r // (2 * ngam)
    g_of = jnp.full((half_rows, 128), gam_ref[0], jnp.int32)
    for k in range(1, ngam):
        g_of = jnp.where(k_of == k, gam_ref[k], g_of)
    hot = jnp.where(l2 == g_of * (2 * nmom) + p_of * 2 + (r & 1), 1.0, 0.0).astype(BF16)
    for ri in range(2):
        lmat[pl.ds(ri * half_rows, half_rows), :] = jnp.dot(hot, tv[ri], preferred_element_type=F32).astype(BF16)

    swap_b.wait_recv()
    bf[...] = bb[...].astype(F32)
    for s in range(4):
        for which in range(2):
            for c in range(3):
                for a in range(2):
                    br = bf.at[which, 0, s, c][pl.ds(a, 16, stride=2), :]
                    bi = bf.at[which, 1, s, c][pl.ds(a, 16, stride=2), :]
                    for p in range(nmom):
                        co, si = cs[0, p:p + 1, :], cs[1, p:p + 1, :]
                        at_row = pl.ds((p * 4 + s) * 64 + a * 32 + which * 16, 16)
                        lh[at_row, pl.ds(c * 128, 128)] = (co * br - si * bi).astype(BF16)
                        lh[at_row, pl.ds((3 + c) * 128, 128)] = (si * br + co * bi).astype(BF16)

    for distance in range(2, REACH + 1):
        @pl.when(z > distance)
        def _():
            hear(down, distance)
    hear(up, 2)
    send_up.wait_recv()
    for which in range(2):
        s, t, alpha, beta = projector(2, -1)[which]
        for sl in blocks:
            h = [(hup_r[0, which, c, sl, :].astype(F32), hup_r[1, which, c, sl, :].astype(F32)) for c in range(3)]
            h = colored(2, False, h)
            for c in range(3):
                other = times_unit(beta, h[c])
                for ri in range(2):
                    wv[ri, s, c, sl, :] += h[c][ri]
                    wv[ri, t, c, sl, :] += other[ri]
    send_dn.wait_recv()
    for which in range(2):
        s, t, alpha, beta = projector(2, 1)[which]
        for sl in blocks:
            start = sl.start
            for c in range(3):
                h = (hdn_r[0, which, c, sl, :].astype(F32), hdn_r[1, which, c, sl, :].astype(F32))
                other = times_unit(beta, h)
                for comp, value in ((s, h), (t, other)):
                    re = ((wv[0, comp, c, sl, :] - value[0]) * 0.5).astype(BF16)
                    im = ((wv[1, comp, c, sl, :] - value[1]) * 0.5).astype(BF16)
                    top, low = pl.ds(comp * rows + start, 16), pl.ds(4 * rows + comp * rows + start, 16)
                    rh[top, pl.ds(c * 128, 128)] = re
                    rh[top, pl.ds((3 + c) * 128, 128)] = im
                    rh[low, pl.ds(c * 128, 128)] = im
                    rh[low, pl.ds((3 + c) * 128, 128)] = -re

    prod = lax.dot_general(lh[...], rh[...], (((1,), (1,)), ((), ())), preferred_element_type=F32)
    for j in range(nmom * 8):
        for ri in range(2):
            rp[ri, pl.ds(j * 40, 32), :] = prod[j * 32:(j + 1) * 32, ri * 128:(ri + 1) * 128]

    def partial(c):
        return [rp.at[ri][pl.ds(c, nmom * 8, stride=40), :] for ri in range(2)]

    centers = crole.shape[1]
    def part(side, m):
        forward_owner = lax.rem(z + jnp.where(side == 0, m, n - m), n)
        return jnp.concatenate(partial(forward_owner), axis=0)

    def post(side, steps, source, target, which):
        peer = {"space": lax.rem(z + jnp.where(side == 0, steps, n - steps), n)}
        return pltpu.make_async_remote_copy(source, target, csend.at[side, which], crecv.at[side, which], device_id=peer, device_id_type=MESH)

    def direct(side):
        return post(side, 1, c1.at[side, pl.ds(centers, 1)], r1.at[side, pl.ds(centers, 1)], 0)

    def near(side, i):
        return post(side, 1, c1.at[side, pl.ds(i, 1)], r1.at[side, pl.ds(i, 1)], 1 + i)

    def far(side, i):
        return post(side, 2, c2.at[side, pl.ds(i, 1)], r2.at[side, pl.ds(i, 1)], 1 + centers + i)

    def passed(side, i):
        to = (0, centers - 1)[i] if i < 2 else i - 1
        steps = STEP * i + 2 if i < 2 else STEP
        return post(side, steps, crole.at[side, pl.ds(i, 1)], r3.at[side, pl.ds(to, 1)], 1 + 2 * centers + i)

    def has_far(side, i):
        m = STEP * i + 4
        return m < n // 2 or (m == n // 2 and side == down)

    levels = range(centers - 1, -1, -1)

    def center(side, i):
        total = part(side, STEP * i + 2)
        near(side, i).wait_recv()
        total = total + r1[side, i].astype(F32)
        if has_far(side, i):
            far(side, i).wait_recv()
            total = total + r2[side, i].astype(F32)
        if 0 < i < centers - 1:
            passed(side, i + 1).wait_recv()
            total = total + r3[side, i].astype(F32)
        crole[side, i] = total.astype(BF16)
        passed(side, i).start()

    for side in range(2):
        c1[side, centers] = part(side, 1).astype(BF16)
        for i in levels:
            c1[side, i] = part(side, STEP * i + 3).astype(BF16)
            if has_far(side, i):
                c2[side, i] = part(side, STEP * i + 4).astype(BF16)
    def hear_late(distance):
        @pl.when(z <= distance)
        def _():
            hear(down, distance)

    for side in range(2):
        direct(side).start()
    for side in range(2):
        if side == down:
            hear_late(2)
        for i in levels:
            if has_far(side, i):
                far(side, i).start()
            near(side, i).start()
    hear(up, 3)
    def inside(i):
        return z >= STEP * (centers - 1 - i if i else 0) + 7

    order = [i for i in levels if i > 2] + [0, 2]

    def inner(i):
        @pl.when(inside(i))
        def _():
            center(up, i)

    for i in order:
        inner(i)
        if i == centers - 1:
            hear(up, 4)
    hear(up, REACH)
    inner(1)
    center(down, 0)
    hear_late(3)
    for i in levels:
        if i > 1:
            center(down, i)
    for distance in range(4, REACH + 1):
        hear_late(distance)
    center(down, 1)
    for i in [*order, 1]:
        @pl.when(jnp.logical_not(inside(i)))
        def _():
            center(up, i)
    total = jnp.concatenate(partial(z), axis=0)
    for side in range(2):
        direct(side).wait_recv()
        passed(side, 0).wait_recv()
        passed(side, 1).wait_recv()
        total = total + r1[side, centers].astype(F32) + r3[side, 0].astype(F32) + r3[side, centers - 1].astype(F32)
    stack = jnp.concatenate([total if s2 == 0 else pltpu.roll(total, 128 - s2 * rows, 1) for s2 in range(4)], axis=0)
    high = stack.astype(BF16)
    low = (stack - high.astype(F32)).astype(BF16)
    mat = lmat[:, 0:stack.shape[0]]
    out = jnp.dot(mat, high, preferred_element_type=F32) + jnp.dot(mat, low, preferred_element_type=F32)
    o_ref[...] = out[:, 0:rows] * scaling
    for side in range(2):
        direct(side).wait_send()
        for i in levels:
            near(side, i).wait_send()
            if has_far(side, i):
                far(side, i).wait_send()
            passed(side, i).wait_send()
    send_up.wait_send()
    send_dn.wait_send()
    swap_b.wait_send()


def solution(mesh):
    n = mesh.shape["space"]

    def body(backward, forward, gauge_links, momenta, gamma_list):
        cols, plane = forward.shape[3], forward.shape[6]
        nmom, ngam = momenta.shape[0], gamma_list.shape[0]
        scaling = 1.0 / math.sqrt(3.0 * plane * n)
        b = backward.transpose(0, 1, 2, 4, 5, 3, 6).reshape(2, 4, 3, cols, plane)
        f = forward.transpose(0, 1, 2, 4, 5, 3, 6).reshape(2, 4, 3, cols, plane)
        u = gauge_links.transpose(1, 2, 3, 4, 5, 0, 6).reshape(27, 2, plane)
        table = jnp.asarray(contraction_table(nmom), BF16)
        half_shape = (2, 2, 3, cols, plane)
        chunk = (nmom * 16, plane)
        n_rows = nmom * 4 * 2 * cols
        any_spec = pl.BlockSpec(memory_space=pltpu.MemorySpace.HBM)
        centers = (n // 2 - 2) // STEP + 1
        out = pl.pallas_call(
            functools.partial(kernel, n, nmom, ngam, scaling),
            out_shape=jax.ShapeDtypeStruct((2 * nmom * ngam * 2, cols), F32),
            in_specs=[any_spec, any_spec, any_spec, any_spec, any_spec, any_spec],
            out_specs=pl.BlockSpec(memory_space=pltpu.VMEM),
            name="insertion",
            scratch_shapes=[
                pltpu.VMEM(f.shape, BF16),
                pltpu.VMEM(u.shape, BF16),
                pltpu.VMEM(table.shape, BF16),
                pltpu.VMEM((2, *b.shape), BF16),
                pltpu.VMEM(f.shape, F32),
                pltpu.VMEM(u.shape, F32),
                pltpu.VMEM((2, *b.shape), F32),
                pltpu.VMEM(f.shape, F32),
                pltpu.VMEM((n_rows, 6 * plane), BF16),
                pltpu.VMEM((8 * cols, 6 * plane), BF16),
                pltpu.VMEM((2, nmom * 8 * 40, plane), F32),
                pltpu.VMEM(half_shape, BF16),
                pltpu.VMEM(half_shape, BF16),
                pltpu.VMEM(half_shape, BF16),
                pltpu.VMEM(half_shape, BF16),
                pltpu.VMEM((2, centers + 1, *chunk), BF16),
                pltpu.VMEM((2, centers, *chunk), BF16),
                pltpu.VMEM((2, centers, *chunk), BF16),
                pltpu.VMEM((2, centers + 1, *chunk), BF16),
                pltpu.VMEM((2, centers, *chunk), BF16),
                pltpu.VMEM((2, centers, *chunk), BF16),
                pltpu.VMEM((2, 8, plane), F32),
                pltpu.VMEM((2 * nmom * ngam * 2, 256), BF16),
                pltpu.SMEM(momenta.shape, jnp.int32),
                pltpu.SMEM(gamma_list.shape, jnp.int32),
                pltpu.SemaphoreType.DMA((6,)),
                pltpu.SemaphoreType.DMA((2,)),
                pltpu.SemaphoreType.DMA((4,)),
                pltpu.SemaphoreType.DMA((2, 1 + 3 * centers)),
                pltpu.SemaphoreType.DMA((2, 1 + 3 * centers)),
                pltpu.SemaphoreType.REGULAR((REACH, 2)),
                pltpu.SemaphoreType.REGULAR,
            ],
            compiler_params=pltpu.CompilerParams(collective_id=0, has_side_effects=True, vmem_limit_bytes=40 * 2**20),
        )(*[pltpu.with_memory_space_constraint(v, pltpu.MemorySpace.HBM) for v in (momenta, gamma_list, b, f, u, table)])
        return out.reshape(2, nmom, ngam, 1, 2, cols)

    in_specs = (
        P("parts", "tm", None, "spin", None, "space", None),
        P("parts", "tm", None, "spin", None, "space", None),
        P("parts", None, None, None, "tm", "space", None),
        P(),
        P(),
    )
    out_specs = P("parts", None, None, "tm", "space", "spin")
    return jax.shard_map(body, mesh=mesh, in_specs=in_specs, out_specs=out_specs, check_vma=False)
```

```python
import functools
import math

import jax
import jax.numpy as jnp
import numpy as np
from jax import lax
from jax.experimental import pallas as pl
from jax.experimental.pallas import tpu as pltpu
from jax.sharding import PartitionSpec as P

MESH = pl.DeviceIdType.MESH
LX = 32
F32 = jnp.float32
BF16 = jnp.bfloat16

STEP = 3
REACH = STEP + 2


def gamma_tables():
    zeros = np.zeros((4, 4))
    gx = np.array([[0, 0, 0, 1j], [0, 0, 1j, 0], [0, -1j, 0, 0], [-1j, 0, 0, 0]])
    gy = np.array([[0, 0, 0, -1], [0, 0, 1, 0], [0, 1, 0, 0], [-1, 0, 0, 0]]) + 0j
    gz = np.array([[0, 0, 1j, 0], [0, 0, 0, -1j], [-1j, 0, 0, 0], [0, 1j, 0, 0]])
    gt = np.array([[0, 0, 1, 0], [0, 0, 0, 1], [1, 0, 0, 0], [0, 1, 0, 0]]) + 0j
    singles = [gx, gy, gz, gt]
    basis = []
    for number in range(16):
        mat = np.eye(4) + 0j
        for which in range(4):
            if number >> which & 1:
                mat = mat @ singles[which]
        basis.append(mat)
    return singles, np.stack(basis)


def contraction_table(nmom):
    _, basis = gamma_tables()
    table = np.zeros((2, 128, 256), np.float32)
    for g in range(16):
        for p in range(nmom):
            for a in range(2):
                row = g * 2 * nmom + p * 2 + a
                for s in range(4):
                    for s2 in range(4):
                        value = basis[g][s, s2]
                        for ri_out, ri_in, coef in ((0, 0, value.real), (0, 1, -value.imag), (1, 0, value.imag), (1, 1, value.real)):
                            table[ri_out, row, ((s2 * 2 + ri_in) * nmom + p) * 8 + s * 2 + a] = coef
    return table


def times_unit(coef, value):
    re, im = value
    if coef == 1:
        return re, im
    if coef == -1:
        return -re, -im
    if coef == 1j:
        return -im, re
    assert coef == -1j
    return im, -re


def plus(x, y):
    return x[0] + y[0], x[1] + y[1]


def projector(mu, sign):
    singles, _ = gamma_tables()
    mat = np.eye(4) + sign * singles[mu]
    result = []
    for s in range(2):
        t = [t for t in (2, 3) if mat[s, t] != 0][0]
        result.append((s, t, complex(mat[s, t]), complex(mat[t, s])))
    return result


def kernel(n, nmom, ngam, scaling,
           mom_hbm, gam_hbm, b_hbm, f_hbm, u_hbm, t_hbm, o_ref,
           fv, uv, tv, bb, ff, uf, bf, wv, lh, rh, rp, hup_s, hup_r, hdn_s, hdn_r, c1, c2, crole, r1, r2, r3, cs, lmat, mom_ref, gam_ref,
           lsem, bsem, hsem, csend, crecv, inside_sem, readyp):
    z = lax.axis_index("space")
    spin = lax.axis_index("spin")
    rows = fv.shape[3]

    load_f = pltpu.make_async_copy(f_hbm, fv, lsem.at[0])
    load_u = pltpu.make_async_copy(u_hbm, uv.at[pl.ds(0, u_hbm.shape[0])], lsem.at[1])
    load_b = pltpu.make_async_copy(b_hbm, bb.at[spin], lsem.at[2])
    load_t = pltpu.make_async_copy(t_hbm, tv, lsem.at[3])
    load_m = pltpu.make_async_copy(mom_hbm, mom_ref, lsem.at[4])
    load_g = pltpu.make_async_copy(gam_hbm, gam_ref, lsem.at[5])
    for copy in (load_f, load_u, load_b, load_t, load_m, load_g):
        copy.start()

    def chip(d):
        return {"space": lax.rem(z + d, n)}

    def tell(sem, d):
        pl.semaphore_signal(sem, inc=1, device_id=chip(d), device_id_type=MESH)

    up, down = 0, 1
    last = z == n - 1
    near_in, two_in = inside_sem.at[0], inside_sem.at[1]
    barrier = pltpu.get_barrier_semaphore()
    def hear(side, distance):
        pl.semaphore_wait(inside_sem.at[distance - 1, side], 1)
        if distance < REACH:
            tell(inside_sem.at[distance, side], n - 1 if side == up else 1)

    up_later = jnp.logical_and(z > 0, jnp.logical_not(last))
    down_later = z < 2

    @pl.when(up_later)
    def _():
        tell(barrier, 1)

    @pl.when(down_later)
    def _():
        tell(barrier, n - 1)

    @pl.when(spin == 1)
    def _():
        pl.semaphore_signal(barrier, inc=1, device_id={"spin": 0}, device_id_type=MESH)

    count = jnp.where(up_later, 0, 1) + jnp.where(down_later, 0, 1) + jnp.where(spin == 0, 1, 0)

    @pl.when(count > 0)
    def _():
        pl.semaphore_wait(barrier, count)

    @pl.when(jnp.logical_not(down_later))
    def _():
        tell(near_in.at[up], n - 1)

    @pl.when(jnp.logical_not(up_later))
    def _():
        tell(near_in.at[down], 1)

    @pl.when(spin == 0)
    def _():
        pl.semaphore_signal(readyp, inc=1, device_id={"spin": 1}, device_id_type=MESH)

    load_f.wait()
    load_u.wait()
    ff[...] = fv[...].astype(F32)
    for i in range(u_hbm.shape[0]):
        uf[i] = uv[i].astype(F32)

    def link(mu, c, d, dagger):
        if dagger:
            return uf[mu * 9 + d * 3 + c, 0:1, :], -uf[mu * 9 + d * 3 + c, 1:2, :]
        return uf[mu * 9 + c * 3 + d, 0:1, :], uf[mu * 9 + c * 3 + d, 1:2, :]

    def colored(mu, dagger, h):
        out = []
        for c in range(3):
            re = im = None
            for d in range(3):
                cr, ci = link(mu, c, d, dagger)
                hr, hi = h[d]
                pr, pi = cr * hr - ci * hi, cr * hi + ci * hr
                re, im = (pr, pi) if re is None else (re + pr, im + pi)
            out.append((re, im))
        return out

    def half(mu, sign, which, sl):
        s, t, alpha, beta = projector(mu, sign)[which]
        h = []
        for c in range(3):
            x = (ff[0, s, c, sl, :], ff[1, s, c, sl, :])
            y = (ff[0, t, c, sl, :], ff[1, t, c, sl, :])
            h.append(plus(x, times_unit(alpha, y)))
        return s, t, beta, h

    blocks = [pl.ds(i, 16) for i in range(0, rows, 16)]
    for which in range(2):
        for sl in blocks:
            _, _, _, h = half(2, -1, which, sl)
            for c in range(3):
                hup_s[0, which, c, sl, :] = h[c][0].astype(BF16)
                hup_s[1, which, c, sl, :] = h[c][1].astype(BF16)
    send_up = pltpu.make_async_remote_copy(hup_s, hup_r, hsem.at[0], hsem.at[1], device_id=chip(n - 1), device_id_type=MESH)
    for which in range(2):
        for sl in blocks:
            _, _, _, h = half(2, 1, which, sl)
            h = colored(2, True, h)
            for c in range(3):
                hdn_s[0, which, c, sl, :] = h[c][0].astype(BF16)
                hdn_s[1, which, c, sl, :] = h[c][1].astype(BF16)
    send_dn = pltpu.make_async_remote_copy(hdn_s, hdn_r, hsem.at[2], hsem.at[3], device_id=chip(1), device_id_type=MESH)

    @pl.when(jnp.logical_not(down_later))
    def _():
        send_up.start()

    @pl.when(up_later)
    def _():
        pl.semaphore_wait(near_in.at[up], 1)

    send_dn.start()

    @pl.when(down_later)
    def _():
        pl.semaphore_wait(near_in.at[down], 1)
        send_up.start()

    tell(two_in.at[up], n - 1)
    tell(two_in.at[down], 1)
    load_b.wait()

    @pl.when(spin == 1)
    def _():
        pl.semaphore_wait(readyp, 1)

    swap_b = pltpu.make_async_remote_copy(bb.at[spin], bb.at[spin], bsem.at[0], bsem.at[1], device_id={"spin": 1 - spin}, device_id_type=MESH)
    swap_b.start()
    load_m.wait()
    sub = lax.broadcasted_iota(jnp.int32, (8, 128), 0)
    lane = lax.broadcasted_iota(jnp.int32, (8, 128), 1)
    x1, x2 = lane & (LX - 1), lane // LX
    width_y = 128 // LX

    def momentum(axis):
        value = jnp.full((8, 128), mom_ref[0, axis], jnp.int32)
        for p in range(1, nmom):
            value = jnp.where(sub == p, mom_ref[p, axis], value)
        return value

    turn = (((momentum(0) * x1) & (LX - 1)).astype(F32) / float(LX)
            + ((momentum(1) * x2) & (width_y - 1)).astype(F32) / float(width_y))
    turn = ((momentum(2) * z) & (n - 1)).astype(F32) / float(n) + turn
    theta = 2.0 * math.pi * turn
    cs[0] = jnp.cos(theta)
    cs[1] = jnp.sin(theta)

    first = lane[0:1, :] & (LX - 1)
    for mu in range(2):
        for which in range(2):
            for sl in blocks:
                for sign in (-1, 1):
                    s, t, beta, h = half(mu, sign, which, sl)
                    if sign == 1:
                        h = colored(mu, True, h)
                    moved = []
                    for pair in h:
                        if mu == 1:
                            moved.append(tuple(pltpu.roll(v, 128 - LX if sign == -1 else LX, 1) for v in pair))
                        elif sign == -1:
                            moved.append(tuple(jnp.where(first == LX - 1, pltpu.roll(v, LX - 1, 1), pltpu.roll(v, 127, 1)) for v in pair))
                        else:
                            moved.append(tuple(jnp.where(first == 0, pltpu.roll(v, 128 - (LX - 1), 1), pltpu.roll(v, 1, 1)) for v in pair))
                    h = moved
                    if sign == -1:
                        h = colored(mu, False, h)
                    for c in range(3):
                        other = times_unit(beta, h[c])
                        for ri in range(2):
                            if mu == 0 and sign == -1:
                                wv[ri, s, c, sl, :] = h[c][ri]
                                wv[ri, t, c, sl, :] = other[ri]
                            elif sign == -1:
                                wv[ri, s, c, sl, :] += h[c][ri]
                                wv[ri, t, c, sl, :] += other[ri]
                            else:
                                wv[ri, s, c, sl, :] -= h[c][ri]
                                wv[ri, t, c, sl, :] -= other[ri]

    load_t.wait()
    load_g.wait()
    half_rows = nmom * ngam * 2
    r = lax.broadcasted_iota(jnp.int32, (half_rows, 128), 0)
    l2 = lax.broadcasted_iota(jnp.int32, (half_rows, 128), 1)
    k_of = (r >> 1) & (ngam - 1)
    p_of = r // (2 * ngam)
    g_of = jnp.full((half_rows, 128), gam_ref[0], jnp.int32)
    for k in range(1, ngam):
        g_of = jnp.where(k_of == k, gam_ref[k], g_of)
    hot = jnp.where(l2 == g_of * (2 * nmom) + p_of * 2 + (r & 1), 1.0, 0.0).astype(BF16)
    for ri in range(2):
        lmat[pl.ds(ri * half_rows, half_rows), :] = jnp.dot(hot, tv[ri], preferred_element_type=F32).astype(BF16)

    swap_b.wait_recv()
    bf[0:2] = bb[...].astype(F32)
    for s in range(4):
        for which in range(2):
            for c in range(3):
                for a in range(2):
                    br = bf.at[which, 0, s, c][pl.ds(a, 16, stride=2), :]
                    bi = bf.at[which, 1, s, c][pl.ds(a, 16, stride=2), :]
                    for p in range(nmom):
                        co, si = cs[0, p:p + 1, :], cs[1, p:p + 1, :]
                        at_row = pl.ds((p * 4 + s) * 64 + a * 32 + which * 16, 16)
                        lh[at_row, pl.ds(c * 128, 128)] = (co * br - si * bi).astype(BF16)
                        lh[at_row, pl.ds((3 + c) * 128, 128)] = (si * br + co * bi).astype(BF16)

    for distance in range(2, REACH + 1):
        @pl.when(z > distance)
        def _():
            hear(down, distance)
    hear(up, 2)
    send_up.wait_recv()
    for which in range(2):
        s, t, alpha, beta = projector(2, -1)[which]
        for sl in blocks:
            h = [(hup_r[0, which, c, sl, :].astype(F32), hup_r[1, which, c, sl, :].astype(F32)) for c in range(3)]
            h = colored(2, False, h)
            for c in range(3):
                other = times_unit(beta, h[c])
                for ri in range(2):
                    wv[ri, s, c, sl, :] += h[c][ri]
                    wv[ri, t, c, sl, :] += other[ri]
    send_dn.wait_recv()
    for which in range(2):
        s, t, alpha, beta = projector(2, 1)[which]
        for sl in blocks:
            start = sl.start
            for c in range(3):
                h = (hdn_r[0, which, c, sl, :].astype(F32), hdn_r[1, which, c, sl, :].astype(F32))
                other = times_unit(beta, h)
                for comp, value in ((s, h), (t, other)):
                    re = ((wv[0, comp, c, sl, :] - value[0]) * 0.5).astype(BF16)
                    im = ((wv[1, comp, c, sl, :] - value[1]) * 0.5).astype(BF16)
                    top, low = pl.ds(comp * rows + start, 16), pl.ds(4 * rows + comp * rows + start, 16)
                    rh[top, pl.ds(c * 128, 128)] = re
                    rh[top, pl.ds((3 + c) * 128, 128)] = im
                    rh[low, pl.ds(c * 128, 128)] = im
                    rh[low, pl.ds((3 + c) * 128, 128)] = -re

    prod = lax.dot_general(lh[...], rh[...], (((1,), (1,)), ((), ())), preferred_element_type=F32)
    for j in range(nmom * 8):
        for ri in range(2):
            rp[ri, pl.ds(j * 40, 32), :] = prod[j * 32:(j + 1) * 32, ri * 128:(ri + 1) * 128]

    def partial(c):
        return [rp.at[ri][pl.ds(c, nmom * 8, stride=40), :] for ri in range(2)]

    centers = crole.shape[1]
    def part(side, m):
        forward_owner = lax.rem(z + jnp.where(side == 0, m, n - m), n)
        return jnp.concatenate(partial(forward_owner), axis=0)

    def post(side, steps, source, target, which):
        peer = {"space": lax.rem(z + jnp.where(side == 0, steps, n - steps), n)}
        return pltpu.make_async_remote_copy(source, target, csend.at[side, which], crecv.at[side, which], device_id=peer, device_id_type=MESH)

    def direct(side):
        return post(side, 1, c1.at[side, pl.ds(centers, 1)], r1.at[side, pl.ds(centers, 1)], 0)

    def near(side, i):
        return post(side, 1, c1.at[side, pl.ds(i, 1)], r1.at[side, pl.ds(i, 1)], 1 + i)

    def far(side, i):
        return post(side, 2, c2.at[side, pl.ds(i, 1)], r2.at[side, pl.ds(i, 1)], 1 + centers + i)

    def passed(side, i):
        to = (0, centers - 1)[i] if i < 2 else i - 1
        steps = STEP * i + 2 if i < 2 else STEP
        return post(side, steps, crole.at[side, pl.ds(i, 1)], r3.at[side, pl.ds(to, 1)], 1 + 2 * centers + i)

    def has_far(side, i):
        m = STEP * i + 4
        return m < n // 2 or (m == n // 2 and side == down)

    levels = range(centers - 1, -1, -1)

    def center(side, i):
        total = part(side, STEP * i + 2)
        near(side, i).wait_recv()
        total = total + r1[side, i].astype(F32)
        if has_far(side, i):
            far(side, i).wait_recv()
            total = total + r2[side, i].astype(F32)
        if 0 < i < centers - 1:
            passed(side, i + 1).wait_recv()
            total = total + r3[side, i].astype(F32)
        crole[side, i] = total.astype(BF16)
        passed(side, i).start()

    for side in range(2):
        c1[side, centers] = part(side, 1).astype(BF16)
        for i in levels:
            c1[side, i] = part(side, STEP * i + 3).astype(BF16)
            if has_far(side, i):
                c2[side, i] = part(side, STEP * i + 4).astype(BF16)
    def hear_late(distance):
        @pl.when(z <= distance)
        def _():
            hear(down, distance)

    for side in range(2):
        direct(side).start()
    for side in range(2):
        if side == down:
            hear_late(2)
        for i in levels:
            if has_far(side, i):
                far(side, i).start()
            near(side, i).start()
    hear(up, 3)
    def inside(i):
        return z >= STEP * (centers - 1 - i if i else 0) + 7

    order = [i for i in levels if i > 2] + [0, 2]

    def inner(i):
        @pl.when(inside(i))
        def _():
            center(up, i)

    for i in order:
        inner(i)
        if i == centers - 1:
            hear(up, 4)
    hear(up, REACH)
    inner(1)
    center(down, 0)
    hear_late(3)
    for i in levels:
        if i > 1:
            center(down, i)
    for distance in range(4, REACH + 1):
        hear_late(distance)
    center(down, 1)
    for i in [*order, 1]:
        @pl.when(jnp.logical_not(inside(i)))
        def _():
            center(up, i)
    total = jnp.concatenate(partial(z), axis=0)
    for side in range(2):
        direct(side).wait_recv()
        passed(side, 0).wait_recv()
        passed(side, 1).wait_recv()
        total = total + r1[side, centers].astype(F32) + r3[side, 0].astype(F32) + r3[side, centers - 1].astype(F32)
    stack = jnp.concatenate([total if s2 == 0 else pltpu.roll(total, 128 - s2 * rows, 1) for s2 in range(4)], axis=0)
    high = stack.astype(BF16)
    low = (stack - high.astype(F32)).astype(BF16)
    mat = lmat[:, 0:stack.shape[0]]
    out = jnp.dot(mat, high, preferred_element_type=F32) + jnp.dot(mat, low, preferred_element_type=F32)
    o_ref[...] = out[:, 0:rows] * scaling
    for side in range(2):
        direct(side).wait_send()
        for i in levels:
            near(side, i).wait_send()
            if has_far(side, i):
                far(side, i).wait_send()
            passed(side, i).wait_send()
    send_up.wait_send()
    send_dn.wait_send()
    swap_b.wait_send()


def solution(mesh):
    n = mesh.shape["space"]

    def body(backward, forward, gauge_links, momenta, gamma_list):
        cols, plane = forward.shape[3], forward.shape[6]
        nmom, ngam = momenta.shape[0], gamma_list.shape[0]
        scaling = 1.0 / math.sqrt(3.0 * plane * n)
        b = backward.transpose(0, 1, 2, 4, 5, 3, 6).reshape(2, 4, 3, cols, plane)
        f = forward.transpose(0, 1, 2, 4, 5, 3, 6).reshape(2, 4, 3, cols, plane)
        u = gauge_links.transpose(1, 2, 3, 4, 5, 0, 6).reshape(27, 2, plane)
        table = jnp.asarray(contraction_table(nmom), BF16)
        half_shape = (2, 2, 3, cols, plane)
        chunk = (nmom * 16, plane)
        n_rows = nmom * 4 * 2 * cols
        any_spec = pl.BlockSpec(memory_space=pltpu.MemorySpace.HBM)
        centers = (n // 2 - 2) // STEP + 1
        out = pl.pallas_call(
            functools.partial(kernel, n, nmom, ngam, scaling),
            out_shape=jax.ShapeDtypeStruct((2 * nmom * ngam * 2, cols), F32),
            in_specs=[any_spec, any_spec, any_spec, any_spec, any_spec, any_spec],
            out_specs=pl.BlockSpec(memory_space=pltpu.VMEM),
            name="insertion",
            scratch_shapes=[
                pltpu.VMEM(f.shape, BF16),
                pltpu.VMEM((u.shape[0] + 9, *u.shape[1:]), BF16),
                pltpu.VMEM(table.shape, BF16),
                pltpu.VMEM((2, *b.shape), BF16),
                pltpu.VMEM(f.shape, F32),
                pltpu.VMEM((u.shape[0] + 9, *u.shape[1:]), F32),
                pltpu.VMEM((3, *b.shape), F32),
                pltpu.VMEM(f.shape, F32),
                pltpu.VMEM((n_rows, 6 * plane), BF16),
                pltpu.VMEM((8 * cols, 6 * plane), BF16),
                pltpu.VMEM((2, nmom * 8 * 40 + 40, plane), F32),
                pltpu.VMEM(half_shape, BF16),
                pltpu.VMEM(half_shape, BF16),
                pltpu.VMEM(half_shape, BF16),
                pltpu.VMEM(half_shape, BF16),
                pltpu.VMEM((2, centers + 1, *chunk), BF16),
                pltpu.VMEM((2, centers, *chunk), BF16),
                pltpu.VMEM((2, centers, *chunk), BF16),
                pltpu.VMEM((2, centers + 1, *chunk), BF16),
                pltpu.VMEM((2, centers, *chunk), BF16),
                pltpu.VMEM((2, centers, *chunk), BF16),
                pltpu.VMEM((3, 8, plane), F32),
                pltpu.VMEM((2 * nmom * ngam * 2, 256), BF16),
                pltpu.SMEM(momenta.shape, jnp.int32),
                pltpu.SMEM(gamma_list.shape, jnp.int32),
                pltpu.SemaphoreType.DMA((6,)),
                pltpu.SemaphoreType.DMA((2,)),
                pltpu.SemaphoreType.DMA((4,)),
                pltpu.SemaphoreType.DMA((2, 1 + 3 * centers)),
                pltpu.SemaphoreType.DMA((2, 1 + 3 * centers)),
                pltpu.SemaphoreType.REGULAR((REACH, 2)),
                pltpu.SemaphoreType.REGULAR,
            ],
            compiler_params=pltpu.CompilerParams(collective_id=0, has_side_effects=True, vmem_limit_bytes=40 * 2**20),
        )(*[pltpu.with_memory_space_constraint(v, pltpu.MemorySpace.HBM) for v in (momenta, gamma_list, b, f, u, table)])
        return out.reshape(2, nmom, ngam, 1, 2, cols)

    in_specs = (
        P("parts", "tm", None, "spin", None, "space", None),
        P("parts", "tm", None, "spin", None, "space", None),
        P("parts", None, None, None, "tm", "space", None),
        P(),
        P(),
    )
    out_specs = P("parts", None, None, "tm", "space", "spin")
    return jax.shard_map(body, mesh=mesh, in_specs=in_specs, out_specs=out_specs, check_vma=False)
```
